8 devices in a mesh: data: 1 (over z), seq: 8 (over y, x, core).
Axes of the slice: x: 2, y: 2, z: 1, core: 2. Of those that a mesh axis runs over, the one named last changes fastest.
Arguments:
- tokens: bfloat16 [2, 256, 1024], P('data', 'seq')
- lengths: int32 [2], P('data')
- slot_param: bfloat16 [1024, 512], replicated
- logit_scale: float32 [], replicated
- w_in: bfloat16 [32, 1024, 4096], P('seq')
- w_out: bfloat16 [32, 4096, 1024], P('seq')
Outputs:
- output: bfloat16 [2, 256, 1024], P('data', 'seq')
All inputs are finite; a program needn't handle non-finite values.
Results may differ from the reference program's by a relative error of at most 0.0131918.
Values are sent between devices in bfloat16 or wider.
A program may use at most 1 GiB of HBM per device.

```python
import jax
import jax.numpy as jnp
from jax import lax

BATCH = 2
TOKENS = 256
D_MODEL = 1024
FF_DIM = 4096
EXPERTS = 32
SLOTS = 16
LATENT = 16

N_SLOTS = EXPERTS * SLOTS
EPSILON = 1e-6
NEG_FILL = -1e30


def setup_inputs(seed: int = 0, part: int = 0) -> dict:
    shared = jax.random.split(jax.random.key(seed), 6)
    own = jax.random.split(jax.random.fold_in(jax.random.key(seed + 1), part), 3)
    basis = jax.random.normal(shared[0], (LATENT, D_MODEL), jnp.float32)
    phi_code = jax.random.normal(shared[1], (LATENT, N_SLOTS), jnp.float32)
    slot_param = jnp.dot(basis.T, phi_code) / LATENT ** 0.5 + 0.5 * jax.random.normal(shared[2], (D_MODEL, N_SLOTS), jnp.float32)
    logit_scale = 6.0 + 4.0 * jax.random.uniform(shared[3], (), jnp.float32)
    w_in = 2.0 * D_MODEL ** -0.5 * jax.random.normal(shared[4], (EXPERTS, D_MODEL, FF_DIM), jnp.float32)
    w_out = 2.0 * FF_DIM ** -0.5 * jax.random.normal(shared[5], (EXPERTS, FF_DIM, D_MODEL), jnp.float32)
    tok_code = jax.random.normal(own[0], (BATCH, TOKENS, LATENT), jnp.float32)
    tokens = jnp.einsum("btl,ld->btd", tok_code, basis) / LATENT ** 0.5 + 0.5 * jax.random.normal(own[1], (BATCH, TOKENS, D_MODEL), jnp.float32)
    drawn = jax.random.randint(own[2], (BATCH,), 1, TOKENS + 1, jnp.int32)
    lengths = jnp.where(jnp.arange(BATCH) == 0, TOKENS, drawn).astype(jnp.int32)
    return {"tokens": tokens.astype(jnp.bfloat16), "lengths": lengths, "slot_param": slot_param.astype(jnp.bfloat16), "logit_scale": logit_scale, "w_in": w_in.astype(jnp.bfloat16), "w_out": w_out.astype(jnp.bfloat16)}


def l2_normed(values, axis_dim):
    v32 = values.astype(jnp.float32)
    return (v32 * lax.rsqrt(jnp.sum(v32 * v32, axis=axis_dim, keepdims=True) + EPSILON)).astype(jnp.bfloat16)


def reference(tokens, lengths, slot_param, logit_scale, w_in, w_out):
    phi_norm = l2_normed(slot_param, 0).astype(jnp.float32)
    positions = jnp.arange(TOKENS, dtype=jnp.int32)

    def row_logits(tok_row):
        tok_norm = l2_normed(tok_row, 1).astype(jnp.float32)
        return logit_scale * jnp.dot(tok_norm, phi_norm, preferred_element_type=jnp.float32)

    def dispatch_row(row_args):
        tok_row, len_row = row_args
        logits = row_logits(tok_row)
        masked = jnp.where((positions < len_row)[:, None], logits, NEG_FILL)
        disp_w = jnp.exp(masked - jnp.max(masked, axis=0, keepdims=True))
        col_sum = jnp.sum(disp_w, axis=0)
        slot_sum = jnp.dot(disp_w.astype(jnp.bfloat16).astype(jnp.float32).T, tok_row.astype(jnp.float32), preferred_element_type=jnp.float32)
        return (slot_sum / col_sum[:, None]).astype(jnp.bfloat16)

    slot_in = lax.map(dispatch_row, (tokens, lengths))
    slot_grp = jnp.transpose(slot_in.reshape(BATCH, EXPERTS, SLOTS, D_MODEL), (1, 0, 2, 3))

    def expert_ffn(exp_args):
        slot_exp, win_exp, wout_exp = exp_args
        hidden = jnp.einsum("bsd,df->bsf", slot_exp.astype(jnp.float32), win_exp.astype(jnp.float32))
        hidden = jax.nn.gelu(hidden).astype(jnp.bfloat16)
        return jnp.einsum("bsf,fd->bsd", hidden.astype(jnp.float32), wout_exp.astype(jnp.float32)).astype(jnp.bfloat16)

    slot_out = lax.map(expert_ffn, (slot_grp, w_in, w_out))
    slot_out = jnp.transpose(slot_out, (1, 0, 2, 3)).reshape(BATCH, N_SLOTS, D_MODEL)

    def combine_row(row_args):
        tok_row, len_row, out_row = row_args
        logits = row_logits(tok_row)
        comb_w = jnp.exp(logits - jnp.max(logits, axis=1, keepdims=True))
        row_sum = jnp.sum(comb_w, axis=1, keepdims=True)
        tok_mixed = jnp.dot(comb_w.astype(jnp.bfloat16).astype(jnp.float32), out_row.astype(jnp.float32), preferred_element_type=jnp.float32) / row_sum
        return jnp.where((positions < len_row)[:, None], tok_mixed, 0.0).astype(jnp.bfloat16)

    return lax.map(combine_row, (tokens, lengths, slot_out))
```

```python
import jax
import jax.numpy as jnp
from jax import lax
from jax.experimental import pallas as pl
from jax.experimental.pallas import tpu as pltpu
from jax.sharding import PartitionSpec as P

EPSILON = 1e-6
NEG_FILL = -1e30
MESH = pl.DeviceIdType.MESH
F32 = jnp.float32
BF16 = jnp.bfloat16


def row_normed(v):
    v32 = v.astype(F32)
    return (v32 * lax.rsqrt(jnp.sum(v32 * v32, axis=-1, keepdims=True) + EPSILON)).astype(BF16)


def layer_kernel(len_ref, g_ref, x_hbm, phi_hbm, w1_hbm, w2_hbm, y_ref,
                 xg, xn, phi_v, pn, pnt, xs, h_v, yg, cw, qs, w1b, w2b,
                 x_sem, phi_sem, w1_sem, w2_sem, w2l_sem,
                 sx_sem, rx_sem, sy_sem, ry_sem):
    batch, tok, d_model = y_ref.shape
    n_exp = w1_hbm.shape[0]
    ff = w1_hbm.shape[2]
    n_slots = phi_hbm.shape[1]
    all_tok = xg.shape[1]
    slots = xs.shape[1]
    per = slots // n_exp
    ring = w1b.shape[0]
    chunks = w2l_sem.shape[0]
    width = d_model // chunks

    me = lax.axis_index("seq")
    core = lax.rem(me, 2)
    chip = lax.div(me, 2)
    part = me + 1 - 2 * core
    xnb = me + 2 - 4 * lax.rem(chip, 2)
    ynb = me + 4 - 8 * lax.div(chip, 2)
    dia = xnb + ynb - me
    flip = 1 - 2 * core
    owners = (part, xnb, ynb, dia, xnb + flip, ynb + flip, dia + flip)

    barrier = pltpu.get_barrier_semaphore()
    for dev in owners[:4]:
        pl.semaphore_signal(barrier, inc=1, device_id={"seq": dev}, device_id_type=MESH)

    def tok_rows(dev):
        return pl.ds(pl.multiple_of(dev * tok, tok), tok)

    own_x = pltpu.make_async_copy(x_hbm, xg.at[:, tok_rows(me), :], x_sem)
    own_x.start()
    own_phi = pltpu.make_async_copy(phi_hbm, phi_v, phi_sem)
    own_phi.start()

    def w1_copy(e):
        return pltpu.make_async_copy(w1_hbm.at[e], w1b.at[lax.rem(e, ring)], w1_sem.at[lax.rem(e, ring)])

    def w2_copy(e):
        return pltpu.make_async_copy(w2_hbm.at[e], w2b.at[lax.rem(e, ring)], w2_sem.at[lax.rem(e, ring)])

    def w2_last(c):
        cols = pl.ds(c * width, width)
        return pltpu.make_async_copy(w2_hbm.at[n_exp - 1, :, cols], w2b.at[(n_exp - 1) % ring, :, cols], w2l_sem.at[c])

    for e in range(ring):
        w1_copy(e).start()
        w2_copy(e).start()

    def x_send(owner, rel, to, k):
        block = xg.at[:, tok_rows(owner), :]
        return pltpu.make_async_remote_copy(src_ref=block, dst_ref=block, send_sem=sx_sem.at[k],
                                            recv_sem=rx_sem.at[rel], device_id={"seq": to}, device_id_type=MESH)

    own_x.wait()
    pl.semaphore_wait(barrier, 4)
    x_sends = [x_send(me, 1, xnb, 1), x_send(me, 2, ynb, 2), x_send(me, 3, dia, 3), x_send(me, 0, part, 0)]
    for copy in x_sends:
        copy.start()

    own_phi.wait()
    for c in range(n_slots // 128):
        cols = pl.ds(c * 128, 128)
        p32 = phi_v[:, cols].astype(F32)
        pn[:, cols] = (p32 * lax.rsqrt(jnp.sum(p32 * p32, axis=0, keepdims=True) + EPSILON)).astype(BF16)
    chip_cols = pl.ds(pl.multiple_of(chip * 128, 128), 128)
    pnt[...] = pn[:, chip_cols].T
    g = g_ref[0, 0]

    def normalise(dev):
        for b in range(batch):
            xn[b, tok_rows(dev), :] = row_normed(xg[b, tok_rows(dev), :])

    normalise(me)
    for b in range(batch):
        own_l = g * jnp.dot(xn[b, tok_rows(me), :], pn[...], preferred_element_type=F32)
        c_exp = jnp.exp(own_l - jnp.max(own_l, axis=1, keepdims=True))
        cw[b] = c_exp.astype(BF16)
        qs[b] = jnp.broadcast_to(jnp.sum(c_exp, axis=1, keepdims=True), qs.shape[1:])

    def x_wait(rel):
        x_send(owners[rel], rel, part, 0).wait_recv()

    x_wait(0)
    normalise(owners[0])
    for rel in (1, 2, 3):
        x_wait(rel)
        fwd = x_send(owners[rel], rel + 3, part, rel + 3)
        fwd.start()
        x_sends.append(fwd)
        normalise(owners[rel])
    for rel in (4, 5, 6):
        x_wait(rel)
        normalise(owners[rel])

    own_pnt = pnt[pl.ds(pl.multiple_of(core * slots, slots), slots), :]
    for b in range(batch):
        lt = g * lax.dot_general(own_pnt, xn[b], (((1,), (1,)), ((), ())), preferred_element_type=F32)
        pos = lax.broadcasted_iota(jnp.int32, lt.shape, 1)
        lt = jnp.where(pos < len_ref[b], lt, NEG_FILL)
        d_exp = jnp.exp(lt - jnp.max(lt, axis=1, keepdims=True))
        z = jnp.sum(d_exp, axis=1, keepdims=True)
        slot_sum = jnp.dot(d_exp.astype(BF16), xg[b], preferred_element_type=F32)
        xs[b] = (slot_sum / z).astype(BF16)

    def y_rows(dev, e):
        return pl.ds(pl.multiple_of(dev * slots + e * per, per), per)

    def y_send(owner, e, rel, to, k, cols=None):
        block = yg.at[:, y_rows(owner, e), :] if cols is None else yg.at[:, y_rows(owner, e), cols]
        return pltpu.make_async_remote_copy(src_ref=block, dst_ref=block, send_sem=sy_sem.at[k],
                                            recv_sem=ry_sem.at[e, rel], device_id={"seq": to}, device_id_type=MESH)

    def send_own(e, cols=None):
        y_send(me, e, 1, xnb, 1, cols).start()
        y_send(me, e, 2, ynb, 2, cols).start()
        y_send(me, e, 3, dia, 3, cols).start()
        y_send(me, e, 0, part, 0, cols).start()

    def y_wait(e, rel):
        y_send(owners[rel], e, rel, part, 0).wait_recv()

    def forward(e):
        for rel in (1, 2, 3):
            y_wait(e, rel)
            y_send(owners[rel], e, rel + 3, part, rel + 3).start()

    fblk = 1024

    def hidden(e, slot):
        rows = xs[:, pl.ds(pl.multiple_of(e * per, per), per), :].reshape(batch * per, d_model)
        for f in range(ff // fblk):
            cols = pl.ds(f * fblk, fblk)
            up = jnp.dot(rows, w1b[slot, :, cols], preferred_element_type=F32)
            h_v[:, cols] = jax.nn.gelu(up).astype(BF16)

    def outputs(e, slot, c):
        cols = pl.ds(c * width, width)
        out = jnp.dot(h_v[...], w2b[slot, :, cols], preferred_element_type=F32).astype(BF16)
        yg[:, y_rows(me, e), cols] = out.reshape(batch, per, width)

    @pl.loop(0, n_exp - 1)
    def _(e):
        w1_copy(e).wait()
        hidden(e, e)
        w2_copy(e).wait()
        for c in range(chunks):
            outputs(e, e, c)
        send_own(e)

        @pl.when(e == 0)
        def _():
            w1_copy(n_exp - 1).start()
            for c in range(chunks):
                w2_last(c).start()

        @pl.when(e > 0)
        def _():
            forward(e - 1)

    last = n_exp - 1
    w1_copy(last).wait()
    hidden(last, last % ring)
    forward(last - 1)
    for c in range(chunks):
        w2_last(c).wait()
        outputs(last, last % ring, c)
        send_own(last, pl.ds(c * width, width))
    forward(last)
    for e in range(n_exp):
        for rel in (0, 4, 5, 6):
            y_wait(e, rel)

    first = me * tok
    for b in range(batch):
        mixed = jnp.dot(cw[b], yg[b], preferred_element_type=F32) / qs[b][:, :1]
        pos = first + lax.broadcasted_iota(jnp.int32, mixed.shape, 0)
        y_ref[b] = jnp.where(pos < len_ref[b], mixed, 0.0).astype(BF16)

    for copy in x_sends:
        copy.wait_send()
    for k in range(7):
        whole = yg.at[:, pl.ds(0, slots), :]
        pltpu.make_async_remote_copy(src_ref=whole, dst_ref=whole, send_sem=sy_sem.at[k], recv_sem=ry_sem.at[0, 0],
                                     device_id={"seq": part}, device_id_type=MESH).wait_send()


def solution(mesh):
    seq_size = mesh.shape["seq"]

    def local_layer(tok_blk, len_blk, slot_param, logit_scale, w_in, w_out):
        batch, tok, d_model = tok_blk.shape
        n_slots = slot_param.shape[1]
        n_exp, _, ff = w_in.shape
        slots = n_slots // seq_size
        ring = n_exp - 1
        chunks = 4
        dma = pltpu.SemaphoreType.DMA
        return pl.pallas_call(
            layer_kernel,
            out_shape=jax.ShapeDtypeStruct((batch, tok, d_model), BF16),
            in_specs=[pl.BlockSpec(memory_space=pltpu.SMEM)] * 2 + [pl.BlockSpec(memory_space=pltpu.HBM)] * 4,
            out_specs=pl.BlockSpec(memory_space=pltpu.VMEM),
            scratch_shapes=[
                pltpu.VMEM((batch, tok * seq_size, d_model), BF16),
                pltpu.VMEM((batch, tok * seq_size, d_model), BF16),
                pltpu.VMEM((d_model, n_slots), BF16),
                pltpu.VMEM((d_model, n_slots), BF16),
                pltpu.VMEM((2 * slots, d_model), BF16),
                pltpu.VMEM((batch, slots, d_model), BF16),
                pltpu.VMEM((batch * slots // n_exp, ff), BF16),
                pltpu.VMEM((batch, n_slots, d_model), BF16),
                pltpu.VMEM((batch, tok, n_slots), BF16),
                pltpu.VMEM((batch, tok, 128), F32),
                pltpu.VMEM((ring, d_model, ff), BF16),
                pltpu.VMEM((ring, ff, d_model), BF16),
                dma, dma, dma((ring,)), dma((ring,)), dma((chunks,)),
                dma((7,)), dma((7,)), dma((7,)), dma((n_exp, 7)),
            ],
            compiler_params=pltpu.CompilerParams(collective_id=0, has_side_effects=True, vmem_limit_bytes=60 * 1024 * 1024),
        )(len_blk, logit_scale.reshape(1, 1), tok_blk, slot_param, w_in, w_out)

    return jax.shard_map(local_layer, mesh=mesh, in_specs=(P("data", "seq", None), P("data"), P(None, None), P(), P("seq", None, None), P("seq", None, None)), out_specs=P("data", "seq", None), check_vma=False)
```

```python
import jax
import jax.numpy as jnp
from jax import lax
from jax.experimental import pallas as pl
from jax.experimental.pallas import tpu as pltpu
from jax.sharding import PartitionSpec as P

EPSILON = 1e-6
NEG_FILL = -1e30
MESH = pl.DeviceIdType.MESH
F32 = jnp.float32
BF16 = jnp.bfloat16


def row_normed(v):
    v32 = v.astype(F32)
    return (v32 * lax.rsqrt(jnp.sum(v32 * v32, axis=-1, keepdims=True) + EPSILON)).astype(BF16)


def layer_kernel(len_hbm, g_hbm, x_hbm, phi_hbm, w1_hbm, w2_hbm, y_ref,
                 xg, xn, phi_v, pn, pnt, xs, h_v, yg, cw, qs, w1b, w2b, len_ref, g_ref,
                 len_sem, g_sem, x_sem, phi_sem, w1_sem, w2_sem, w2l_sem,
                 sx_sem, rx_sem, sy_sem, ry_sem, rl_sem):
    batch, tok, d_model = y_ref.shape
    n_exp = w1_hbm.shape[0]
    ff = w1_hbm.shape[2]
    n_slots = phi_hbm.shape[1]
    all_tok = xg.shape[1]
    slots = xs.shape[1]
    per = slots // n_exp
    ring = w1b.shape[0]
    chunks = w2l_sem.shape[0]
    width = d_model // chunks

    me = lax.axis_index("seq")
    core = lax.rem(me, 2)
    chip = lax.div(me, 2)
    part = me + 1 - 2 * core
    xnb = me + 2 - 4 * lax.rem(chip, 2)
    ynb = me + 4 - 8 * lax.div(chip, 2)
    dia = xnb + ynb - me
    flip = 1 - 2 * core
    owners = (part, xnb, ynb, dia, xnb + flip, ynb + flip, dia + flip)

    barrier = pltpu.get_barrier_semaphore()
    for dev in owners[:3]:
        pl.semaphore_signal(barrier, inc=1, device_id={"seq": dev}, device_id_type=MESH)

    def tok_rows(dev):
        return pl.ds(pl.multiple_of(dev * tok, tok), tok)

    own_x = pltpu.make_async_copy(x_hbm, xg.at[:, tok_rows(me), :], x_sem)
    own_x.start()
    own_phi = pltpu.make_async_copy(phi_hbm, phi_v, phi_sem)
    own_phi.start()
    own_len = pltpu.make_async_copy(len_hbm, len_ref, len_sem)
    own_len.start()
    own_g = pltpu.make_async_copy(g_hbm, g_ref, g_sem)
    own_g.start()

    def w1_copy(e):
        return pltpu.make_async_copy(w1_hbm.at[e], w1b.at[lax.rem(e, ring)], w1_sem.at[lax.rem(e, ring)])

    def w2_copy(e):
        return pltpu.make_async_copy(w2_hbm.at[e], w2b.at[lax.rem(e, ring)], w2_sem.at[lax.rem(e, ring)])

    def w2_last(c):
        cols = pl.ds(c * width, width)
        return pltpu.make_async_copy(w2_hbm.at[n_exp - 1, :, cols], w2b.at[(n_exp - 1) % ring, :, cols], w2l_sem.at[c])

    for e in range(ring):
        w1_copy(e).start(priority=1)
        w2_copy(e).start(priority=1)

    def x_send(owner, half, rel, to, k):
        block = xg.at[half, tok_rows(owner), :]
        return pltpu.make_async_remote_copy(src_ref=block, dst_ref=block, send_sem=sx_sem.at[k, half],
                                            recv_sem=rx_sem.at[rel, half], device_id={"seq": to}, device_id_type=MESH)

    own_x.wait()
    pl.semaphore_wait(barrier, 3)
    x_sends = [x_send(me, 0, 1, xnb, 1), x_send(me, 1, 2, ynb, 2), x_send(me, 1, 1, xnb, 1),
               x_send(me, 0, 2, ynb, 2), x_send(me, 0, 0, part, 0), x_send(me, 1, 0, part, 0)]
    for copy in x_sends:
        copy.start()

    own_phi.wait()
    for c in range(n_slots // 128):
        cols = pl.ds(c * 128, 128)
        p32 = phi_v[:, cols].astype(F32)
        pn[:, cols] = (p32 * lax.rsqrt(jnp.sum(p32 * p32, axis=0, keepdims=True) + EPSILON)).astype(BF16)
    chip_cols = pl.ds(pl.multiple_of(chip * 128, 128), 128)
    pnt[...] = pn[:, chip_cols].T
    own_g.wait()
    own_len.wait()
    g = g_ref[0]

    def normalise(dev, half):
        xn[half, tok_rows(dev), :] = row_normed(xg[half, tok_rows(dev), :])

    normalise(me, 0)
    normalise(me, 1)
    for b in range(batch):
        own_l = g * jnp.dot(xn[b, tok_rows(me), :], pn[...], preferred_element_type=F32)
        c_exp = jnp.exp(own_l - jnp.max(own_l, axis=1, keepdims=True))
        cw[b] = c_exp.astype(BF16)
        qs[b] = jnp.broadcast_to(jnp.sum(c_exp, axis=1, keepdims=True), qs.shape[1:])

    def x_wait(rel, half):
        x_send(owners[rel], half, rel, part, 0).wait_recv()

    def x_pass(rel, half, to_rel, to, k):
        copy = x_send(owners[rel], half, to_rel, to, k)
        copy.start()
        x_sends.append(copy)

    x_wait(1, 0)
    x_pass(1, 0, 3, ynb, 3)
    x_pass(1, 0, 4, part, 4)
    x_wait(2, 1)
    x_pass(2, 1, 3, xnb, 3)
    x_pass(2, 1, 5, part, 5)
    normalise(owners[1], 0)
    normalise(owners[2], 1)
    for half in (0, 1):
        x_wait(0, half)
        normalise(owners[0], half)
    x_wait(1, 1)
    x_pass(1, 1, 4, part, 4)
    x_wait(2, 0)
    x_pass(2, 0, 5, part, 5)
    normalise(owners[1], 1)
    normalise(owners[2], 0)
    for rel, half in ((4, 0), (5, 1), (4, 1), (5, 0)):
        x_wait(rel, half)
        normalise(owners[rel], half)
    for half in (0, 1):
        x_wait(3, half)
        x_pass(3, half, 6, part, 6)
    for half in (0, 1):
        normalise(owners[3], half)
    for half in (0, 1):
        x_wait(6, half)
        normalise(owners[6], half)

    own_pnt = pnt[pl.ds(pl.multiple_of(core * slots, slots), slots), :]
    for b in range(batch):
        lt = g * lax.dot_general(own_pnt, xn[b], (((1,), (1,)), ((), ())), preferred_element_type=F32)
        pos = lax.broadcasted_iota(jnp.int32, lt.shape, 1)
        lt = jnp.where(pos < len_ref[b], lt, NEG_FILL)
        d_exp = jnp.exp(lt - jnp.max(lt, axis=1, keepdims=True))
        z = jnp.sum(d_exp, axis=1, keepdims=True)
        slot_sum = jnp.dot(d_exp.astype(BF16), xg[b], preferred_element_type=F32)
        xs[b] = (slot_sum / z).astype(BF16)

    def y_rows(dev, e):
        return pl.ds(pl.multiple_of(dev * slots + e * per, per), per)

    everything = slice(None)

    def y_send(owner, e, to, send, recv, halves=everything, cols=everything):
        block = yg.at[halves, y_rows(owner, e), cols]
        return pltpu.make_async_remote_copy(src_ref=block, dst_ref=block, send_sem=send, recv_sem=recv,
                                            device_id={"seq": to}, device_id_type=MESH)

    def send_own(e):
        y_send(me, e, xnb, sy_sem.at[1], ry_sem.at[e, 1]).start()
        y_send(me, e, ynb, sy_sem.at[2], ry_sem.at[e, 2]).start()
        y_send(me, e, part, sy_sem.at[0], ry_sem.at[e, 0]).start()

    def y_wait(e, rel):
        y_send(owners[rel], e, part, sy_sem.at[0], ry_sem.at[e, rel]).wait_recv()

    def near(e):
        y_wait(e, 1)
        y_send(owners[1], e, ynb, sy_sem.at[7], ry_sem.at[e, 3], halves=pl.ds(0, 1)).start()
        y_send(owners[1], e, part, sy_sem.at[4], ry_sem.at[e, 4]).start()
        y_wait(e, 2)
        y_send(owners[2], e, xnb, sy_sem.at[8], ry_sem.at[e, 3], halves=pl.ds(1, 1)).start()
        y_send(owners[2], e, part, sy_sem.at[5], ry_sem.at[e, 5]).start()

    def far(e):
        y_wait(e, 3)
        y_send(owners[3], e, part, sy_sem.at[6], ry_sem.at[e, 6]).start()

    def last_send(owner, c, rel, to, k):
        return y_send(owner, last, to, sy_sem.at[k], rl_sem.at[c, rel], cols=pl.ds(c * width, width))

    last = n_exp - 1
    fblk = 1024

    def hidden(e, slot):
        rows = xs[:, pl.ds(pl.multiple_of(e * per, per), per), :].reshape(batch * per, d_model)
        for f in range(ff // fblk):
            cols = pl.ds(f * fblk, fblk)
            up = jnp.dot(rows, w1b[slot, :, cols], preferred_element_type=F32)
            h_v[:, cols] = jax.nn.gelu(up).astype(BF16)

    def outputs(e, slot, c):
        cols = pl.ds(c * width, width)
        out = jnp.dot(h_v[...], w2b[slot, :, cols], preferred_element_type=F32).astype(BF16)
        yg[:, y_rows(me, e), cols] = out.reshape(batch, per, width)

    @pl.loop(0, n_exp - 1)
    def _(e):
        w1_copy(e).wait()
        hidden(e, e)
        w2_copy(e).wait()
        for c in range(chunks):
            outputs(e, e, c)
        send_own(e)

        @pl.when(e == 0)
        def _():
            w1_copy(last).start(priority=1)
            for c in range(chunks):
                w2_last(c).start(priority=1)

        @pl.when(e > 0)
        def _():
            near(e - 1)

        @pl.when(e > 1)
        def _():
            far(e - 2)

    w1_copy(last).wait()
    hidden(last, last % ring)
    for c in range(chunks):
        w2_last(c).wait()
        outputs(last, last % ring, c)
        last_send(me, c, 1, xnb, 1).start()
        last_send(me, c, 2, ynb, 2).start()
        last_send(me, c, 3, dia, 3).start()
        last_send(me, c, 0, part, 0).start()
        if c == 0:
            far(last - 2)
            near(last - 1)
    far(last - 1)
    for c in range(chunks):
        for rel in (1, 2, 3):
            last_send(owners[rel], c, rel, part, 0).wait_recv()
            last_send(owners[rel], c, rel + 3, part, rel + 3).start()
    for e in range(last):
        for rel in (0, 4, 5, 6):
            y_wait(e, rel)
    for c in range(chunks):
        for rel in (0, 4, 5, 6):
            last_send(owners[rel], c, rel, part, 0).wait_recv()

    first = me * tok
    for b in range(batch):
        mixed = jnp.dot(cw[b], yg[b], preferred_element_type=F32) / qs[b][:, :1]
        pos = first + lax.broadcasted_iota(jnp.int32, mixed.shape, 0)
        y_ref[b] = jnp.where(pos < len_ref[b], mixed, 0.0).astype(BF16)

    for copy in x_sends:
        copy.wait_send()
    for k in range(9):
        if k == 3:
            sent = yg.at[:, pl.ds(0, per), :]
        elif k > 6:
            sent = yg.at[0, pl.ds(0, last * per), :]
        else:
            sent = yg.at[:, pl.ds(0, slots), :]
        pltpu.make_async_remote_copy(src_ref=sent, dst_ref=sent, send_sem=sy_sem.at[k], recv_sem=ry_sem.at[0, 0],
                                     device_id={"seq": part}, device_id_type=MESH).wait_send()


def solution(mesh):
    seq_size = mesh.shape["seq"]

    def local_layer(tok_blk, len_blk, slot_param, logit_scale, w_in, w_out):
        batch, tok, d_model = tok_blk.shape
        n_slots = slot_param.shape[1]
        n_exp, _, ff = w_in.shape
        slots = n_slots // seq_size
        ring = n_exp - 1
        chunks = 4
        dma = pltpu.SemaphoreType.DMA
        return pl.pallas_call(
            layer_kernel,
            out_shape=jax.ShapeDtypeStruct((batch, tok, d_model), BF16),
            in_specs=[pl.BlockSpec(memory_space=pltpu.HBM)] * 6,
            out_specs=pl.BlockSpec(memory_space=pltpu.VMEM),
            scratch_shapes=[
                pltpu.VMEM((batch, tok * seq_size, d_model), BF16),
                pltpu.VMEM((batch, tok * seq_size, d_model), BF16),
                pltpu.VMEM((d_model, n_slots), BF16),
                pltpu.VMEM((d_model, n_slots), BF16),
                pltpu.VMEM((2 * slots, d_model), BF16),
                pltpu.VMEM((batch, slots, d_model), BF16),
                pltpu.VMEM((batch * slots // n_exp, ff), BF16),
                pltpu.VMEM((batch, n_slots, d_model), BF16),
                pltpu.VMEM((batch, tok, n_slots), BF16),
                pltpu.VMEM((batch, tok, 128), F32),
                pltpu.VMEM((ring, d_model, ff), BF16),
                pltpu.VMEM((ring, ff, d_model), BF16),
                pltpu.SMEM((batch,), jnp.int32),
                pltpu.SMEM((1,), F32),
                dma, dma, dma, dma, dma((ring,)), dma((ring,)), dma((chunks,)),
                dma((7, 2)), dma((7, 2)), dma((9,)), dma((n_exp, 7)), dma((chunks, 7)),
            ],
            compiler_params=pltpu.CompilerParams(collective_id=0, has_side_effects=True, vmem_limit_bytes=60 * 1024 * 1024),
        )(len_blk, logit_scale.reshape(1), tok_blk, slot_param, w_in, w_out)

    return jax.shard_map(local_layer, mesh=mesh, in_specs=(P("data", "seq", None), P("data"), P(None, None), P(), P("seq", None, None), P("seq", None, None)), out_specs=P("data", "seq", None), check_vma=False)
```

```python
import functools

import jax
import jax.numpy as jnp
from jax import lax
from jax.experimental import pallas as pl
from jax.experimental.pallas import tpu as pltpu
from jax.sharding import PartitionSpec as P

EPSILON = 1e-6
NEG_FILL = -1e30
MESH = pl.DeviceIdType.MESH
F32 = jnp.float32
BF16 = jnp.bfloat16


def row_normed(v):
    v32 = v.astype(F32)
    return (v32 * lax.rsqrt(jnp.sum(v32 * v32, axis=-1, keepdims=True) + EPSILON)).astype(BF16)


def layer_kernel(sems, *refs):
    pl.run_scoped(lambda *scoped: layer_body(*refs, *scoped), *sems)


def layer_body(len_hbm, g_hbm, x_hbm, phi_hbm, w1_hbm, w2_hbm, y_ref,
                 xg, xn, phi_v, pn, pnt, xs, h_v, yg, cw, qs, w1b, w2b, len_ref, g_ref,
                 len_sem, g_sem, x_sem, phi_sem, w1_sem, w2_sem, w2l_sem,
                 sx_sem, rx_sem, sy_sem, ry_sem, rl_sem):
    batch, tok, d_model = y_ref.shape
    n_exp = w1_hbm.shape[0]
    ff = w1_hbm.shape[2]
    n_slots = phi_hbm.shape[1]
    all_tok = xg.shape[1]
    slots = xs.shape[1]
    per = slots // n_exp
    ring = w1b.shape[0]
    chunks = w2l_sem.shape[0]
    width = d_model // chunks
    last = n_exp - 1

    me = lax.axis_index("seq")
    core = lax.rem(me, 2)
    chip = lax.div(me, 2)
    part = me + 1 - 2 * core
    xsame = me + 2 - 4 * lax.rem(chip, 2)
    ysame = me + 4 - 8 * lax.div(chip, 2)
    dsame = xsame + ysame - me
    flip = 1 - 2 * core
    xnb, ynb, dia = xsame + flip, ysame + flip, dsame + flip
    owners = (part, xnb, ynb, dsame, xsame, ysame, dia)
    last_owners = (part, xnb, ynb, dia, xsame, ysame, dsame)

    barrier = pltpu.get_barrier_semaphore()
    for dev in owners[:3]:
        pl.semaphore_signal(barrier, inc=1, device_id={"seq": dev}, device_id_type=MESH)

    def tok_rows(dev):
        return pl.ds(pl.multiple_of(dev * tok, tok), tok)

    own_x = pltpu.make_async_copy(x_hbm, xg.at[:, tok_rows(me), :], x_sem)
    own_x.start()
    own_phi = pltpu.make_async_copy(phi_hbm, phi_v, phi_sem)
    own_phi.start()
    own_len = pltpu.make_async_copy(len_hbm, len_ref, len_sem)
    own_len.start()
    own_g = pltpu.make_async_copy(g_hbm, g_ref, g_sem)
    own_g.start()

    def w1_copy(e):
        return pltpu.make_async_copy(w1_hbm.at[e], w1b.at[lax.rem(e, ring)], w1_sem.at[lax.rem(e, ring)])

    def w2_copy(e):
        return pltpu.make_async_copy(w2_hbm.at[e], w2b.at[lax.rem(e, ring)], w2_sem.at[lax.rem(e, ring)])

    def w2_last(c):
        cols = pl.ds(c * width, width)
        return pltpu.make_async_copy(w2_hbm.at[n_exp - 1, :, cols], w2b.at[(n_exp - 1) % ring, :, cols], w2l_sem.at[c])

    for e in range(ring):
        w1_copy(e).start(priority=1)
        w2_copy(e).start(priority=1)

    quarter = tok // 2

    def x_block(owner, piece):
        return (piece // 2, pl.ds(pl.multiple_of(owner * tok + (piece % 2) * quarter, quarter), quarter))

    def x_send(owner, piece, rel, to, k):
        half, rows = x_block(owner, piece)
        block = xg.at[half, rows, :]
        return pltpu.make_async_remote_copy(src_ref=block, dst_ref=block, send_sem=sx_sem.at[k, piece],
                                            recv_sem=rx_sem.at[rel, piece], device_id={"seq": to}, device_id_type=MESH)

    own_x.wait()
    pl.semaphore_wait(barrier, 3)
    x_sends = []

    def x_start(owner, piece, rel, to, k):
        copy = x_send(owner, piece, rel, to, k)
        copy.start()
        x_sends.append(copy)

    for piece in range(4):
        x_start(me, piece, 1, xnb, 1)
        x_start(me, (piece + 2) % 4, 2, ynb, 2)
    for piece in range(4):
        x_start(me, piece, 0, part, 0)

    own_phi.wait()
    for c in range(n_slots // 128):
        cols = pl.ds(c * 128, 128)
        p32 = phi_v[:, cols].astype(F32)
        pn[:, cols] = (p32 * lax.rsqrt(jnp.sum(p32 * p32, axis=0, keepdims=True) + EPSILON)).astype(BF16)
    chip_cols = pl.ds(pl.multiple_of(chip * 128, 128), 128)
    pnt[...] = pn[:, chip_cols].T
    own_g.wait()
    own_len.wait()
    g = g_ref[0]

    def normalise(dev, piece):
        half, rows = x_block(dev, piece)
        xn[half, rows, :] = row_normed(xg[half, rows, :])

    for piece in range(4):
        normalise(me, piece)
    for b in range(batch):
        own_l = g * jnp.dot(xn[b, tok_rows(me), :], pn[...], preferred_element_type=F32)
        c_exp = jnp.exp(own_l - jnp.max(own_l, axis=1, keepdims=True))
        cw[b] = c_exp.astype(BF16)
        qs[b] = jnp.broadcast_to(jnp.sum(c_exp, axis=1, keepdims=True), qs.shape[1:])

    def x_wait(rel, piece):
        x_send(owners[rel], piece, rel, part, 0).wait_recv()

    for piece in (0, 1):
        x_wait(1, piece)
        x_start(owners[1], piece, 3, ynb, 3)
        x_start(owners[1], piece, 4, part, 4)
        x_wait(2, piece + 2)
        x_start(owners[2], piece + 2, 3, xnb, 3)
        x_start(owners[2], piece + 2, 5, part, 5)
    for piece in range(4):
        x_wait(0, piece)
        normalise(owners[0], piece)
    for piece in (0, 1):
        normalise(owners[1], piece)
        normalise(owners[2], piece + 2)
        x_wait(1, piece + 2)
        x_start(owners[1], piece + 2, 4, part, 4)
        x_wait(2, piece)
        x_start(owners[2], piece, 5, part, 5)
        normalise(owners[1], piece + 2)
        normalise(owners[2], piece)
    for piece in (0, 1):
        x_wait(4, piece)
        normalise(owners[4], piece)
        x_wait(5, piece + 2)
        normalise(owners[5], piece + 2)
    for piece in (0, 2, 1, 3):
        x_wait(3, piece)
        x_start(owners[3], piece, 6, part, 6)
        normalise(owners[3], piece)
    for piece in (0, 1):
        x_wait(4, piece + 2)
        normalise(owners[4], piece + 2)
        x_wait(5, piece)
        normalise(owners[5], piece)
    for piece in (0, 2, 1, 3):
        x_wait(6, piece)
        normalise(owners[6], piece)

    own_pnt = pnt[pl.ds(pl.multiple_of(core * slots, slots), slots), :]
    for b in range(batch):
        lt = g * lax.dot_general(own_pnt, xn[b], (((1,), (1,)), ((), ())), preferred_element_type=F32)
        pos = lax.broadcasted_iota(jnp.int32, lt.shape, 1)
        lt = jnp.where(pos < len_ref[b], lt, NEG_FILL)
        d_exp = jnp.exp(lt - jnp.max(lt, axis=1, keepdims=True))
        z = jnp.sum(d_exp, axis=1, keepdims=True)
        slot_sum = jnp.dot(d_exp.astype(BF16), xg[b], preferred_element_type=F32)
        xs[b] = (slot_sum / z).astype(BF16)

    def y_rows(dev, e):
        return pl.ds(pl.multiple_of(dev * slots + e * per, per), per)

    def y_send(owner, e, rel, to, recv, cols=slice(None)):
        block = yg.at[:, y_rows(owner, e), cols]
        return pltpu.make_async_remote_copy(src_ref=block, dst_ref=block, send_sem=sy_sem.at[rel], recv_sem=recv,
                                            device_id={"seq": to}, device_id_type=MESH)

    def y_chunk(owner, e, c, rel, to, recv):
        return y_send(owner, e, rel, to, recv, pl.ds(c * width, width))

    def send_own(e, cols, recvs):
        for rel, to in ((3, dia), (1, xnb), (2, ynb), (0, part)):
            y_send(me, e, rel, to, recvs.at[rel], cols).start()

    def y_wait(e, rel):
        y_send(last_owners[rel], e, rel, part, ry_sem.at[e, rel]).wait_recv()

    def forward(e):
        for rel in (1, 2, 3):
            y_wait(e, rel)
            y_send(last_owners[rel], e, rel + 3, part, ry_sem.at[e, rel + 3]).start()

    fblk = 1024

    def hidden(e, slot):
        rows = xs[:, pl.ds(pl.multiple_of(e * per, per), per), :].reshape(batch * per, d_model)
        for f in range(ff // fblk):
            cols = pl.ds(f * fblk, fblk)
            up = jnp.dot(rows, w1b[slot, :, cols], preferred_element_type=F32)
            h_v[:, cols] = jax.nn.gelu(up).astype(BF16)

    def outputs(e, slot, cols):
        out = jnp.dot(h_v[...], w2b[slot, :, cols], preferred_element_type=F32).astype(BF16)
        yg[:, y_rows(me, e), cols] = out.reshape(batch, per, cols.size)

    @pl.loop(0, n_exp - 1)
    def _(e):
        w1_copy(e).wait()
        hidden(e, e)

        @pl.when(e == 0)
        def _():
            w1_copy(last).start(priority=1)

        w2_copy(e).wait()
        for c in range(2):
            outputs(e, e, pl.ds(c * 2 * width, 2 * width))
            send_own(e, pl.ds(c * 2 * width, 2 * width), ry_sem.at[e])

        @pl.when(e == 0)
        def _():
            for c in range(chunks):
                w2_last(c).start(priority=1)

        @pl.when(e > 0)
        def _():
            forward(e - 1)

    w1_copy(last).wait()
    hidden(last, last % ring)
    for c in range(chunks):
        w2_last(c).wait()
        outputs(last, last % ring, pl.ds(c * width, width))
        send_own(last, pl.ds(c * width, width), rl_sem.at[c])
    forward(last - 1)
    for c in range(chunks):
        for rel in (1, 2, 3):
            y_chunk(last_owners[rel], last, c, rel, part, rl_sem.at[c, rel]).wait_recv()
            y_chunk(last_owners[rel], last, c, rel + 3, part, rl_sem.at[c, rel + 3]).start()
    for e in range(last):
        for rel in (0, 4, 5, 6):
            y_wait(e, rel)
    for c in range(chunks):
        for rel in (0, 4, 5, 6):
            y_chunk(last_owners[rel], last, c, rel, part, rl_sem.at[c, rel]).wait_recv()

    first = me * tok
    for b in range(batch):
        mixed = jnp.dot(cw[b], yg[b], preferred_element_type=F32) / qs[b][:, :1]
        pos = first + lax.broadcasted_iota(jnp.int32, mixed.shape, 0)
        y_ref[b] = jnp.where(pos < len_ref[b], mixed, 0.0).astype(BF16)

    for copy in x_sends:
        copy.wait_send()
    for rel in range(7):
        sent = yg.at[:, pl.ds(0, slots), :]
        pltpu.make_async_remote_copy(src_ref=sent, dst_ref=sent, send_sem=sy_sem.at[rel], recv_sem=ry_sem.at[0, rel],
                                     device_id={"seq": part}, device_id_type=MESH).wait_send()


def solution(mesh):
    seq_size = mesh.shape["seq"]

    def local_layer(tok_blk, len_blk, slot_param, logit_scale, w_in, w_out):
        batch, tok, d_model = tok_blk.shape
        n_slots = slot_param.shape[1]
        n_exp, _, ff = w_in.shape
        slots = n_slots // seq_size
        ring = n_exp - 1
        chunks = 4
        dma = pltpu.SemaphoreType.DMA
        sems = (dma, dma, dma, dma, dma((ring,)), dma((ring,)), dma((chunks,)),
                dma((7, 4)), dma((7, 4)), dma((7,)), dma((n_exp, 7)), dma((chunks, 7)))
        return pl.pallas_call(
            functools.partial(layer_kernel, sems),
            out_shape=pltpu.VMEM((batch, tok, d_model), BF16),
            in_specs=[pl.BlockSpec(memory_space=pltpu.HBM)] * 6,
            out_specs=pl.BlockSpec(memory_space=pltpu.VMEM),
            scratch_shapes=[
                pltpu.VMEM((batch, tok * seq_size, d_model), BF16),
                pltpu.VMEM((batch, tok * seq_size, d_model), BF16),
                pltpu.VMEM((d_model, n_slots), BF16),
                pltpu.VMEM((d_model, n_slots), BF16),
                pltpu.VMEM((2 * slots, d_model), BF16),
                pltpu.VMEM((batch, slots, d_model), BF16),
                pltpu.VMEM((batch * slots // n_exp, ff), BF16),
                pltpu.VMEM((batch, n_slots, d_model), BF16),
                pltpu.VMEM((batch, tok, n_slots), BF16),
                pltpu.VMEM((batch, tok, 128), F32),
                pltpu.VMEM((ring, d_model, ff), BF16),
                pltpu.VMEM((ring, ff, d_model), BF16),
                pltpu.SMEM((batch,), jnp.int32),
                pltpu.SMEM((1,), F32),
            ],
            compiler_params=pltpu.CompilerParams(collective_id=0, has_side_effects=True, vmem_limit_bytes=60 * 1024 * 1024),
        )(len_blk, logit_scale.reshape(1), tok_blk, slot_param, w_in, w_out)

    return jax.shard_map(local_layer, mesh=mesh, in_specs=(P("data", "seq", None), P("data"), P(None, None), P(), P("seq", None, None), P("seq", None, None)), out_specs=P("data", "seq", None), check_vma=False)
```

```python
import functools

import jax
import jax.numpy as jnp
from jax import lax
from jax.experimental import pallas as pl
from jax.experimental.pallas import tpu as pltpu
from jax.sharding import PartitionSpec as P

EPSILON = 1e-6
NEG_FILL = -1e30
MESH = pl.DeviceIdType.MESH
F32 = jnp.float32
BF16 = jnp.bfloat16


def row_normed(v):
    v32 = v.astype(F32)
    return (v32 * lax.rsqrt(jnp.sum(v32 * v32, axis=-1, keepdims=True) + EPSILON)).astype(BF16)


def layer_kernel(sems, *refs):
    pl.run_scoped(lambda *scoped: layer_body(*refs, *scoped), *sems)


def layer_body(len_hbm, g_hbm, x_hbm, phi_hbm, w1_hbm, w2_hbm, y_ref,
                 xg, xn, la, phi_v, pn, pnt, xs, h_v, yg, cw, qs, w1b, w2b, len_ref, g_ref,
                 len_sem, g_sem, x_sem, phi_sem, w1_sem, w2_sem, w2l_sem,
                 sx_sem, rx_sem, sy_sem, ry_sem, rl_sem):
    batch, tok, d_model = y_ref.shape
    n_exp = w1_hbm.shape[0]
    ff = w1_hbm.shape[2]
    n_slots = phi_hbm.shape[1]
    slots = xs.shape[1]
    per = slots // n_exp
    ring = w1b.shape[0]
    chunks = w2l_sem.shape[0]
    width = d_model // chunks
    last = n_exp - 1

    me = lax.axis_index("seq")
    core = lax.rem(me, 2)
    chip = lax.div(me, 2)
    part = me + 1 - 2 * core
    xsame = me + 2 - 4 * lax.rem(chip, 2)
    ysame = me + 4 - 8 * lax.div(chip, 2)
    dsame = xsame + ysame - me
    flip = 1 - 2 * core
    xnb, ynb, dia = xsame + flip, ysame + flip, dsame + flip
    owners = (part, xnb, ynb, dsame, xsame, ysame, dia)
    last_owners = (part, xnb, ynb, dia, xsame, ysame, dsame)

    barrier = pltpu.get_barrier_semaphore()
    for dev in owners[:3]:
        pl.semaphore_signal(barrier, inc=1, device_id={"seq": dev}, device_id_type=MESH)

    quarter = tok // 2
    slot_of = (1, 2, 3, 6, 4, 5, 7)

    def x_block(slot, piece):
        return xg.at[piece // 2, slot, pl.ds((piece % 2) * quarter, quarter), :]

    def own_x(piece):
        rows = pl.ds((piece % 2) * quarter, quarter)
        return pltpu.make_async_copy(x_hbm.at[piece // 2, rows, :], x_block(0, piece), x_sem.at[piece])

    for piece in (0, 2, 1, 3):
        own_x(piece).start()
    own_phi = pltpu.make_async_copy(phi_hbm, phi_v, phi_sem)
    own_phi.start()
    own_len = pltpu.make_async_copy(len_hbm, len_ref, len_sem)
    own_len.start()
    own_g = pltpu.make_async_copy(g_hbm, g_ref, g_sem)
    own_g.start()

    def w1_copy(e):
        return pltpu.make_async_copy(w1_hbm.at[e], w1b.at[lax.rem(e, ring)], w1_sem.at[lax.rem(e, ring)])

    def w2_copy(e):
        return pltpu.make_async_copy(w2_hbm.at[e], w2b.at[lax.rem(e, ring)], w2_sem.at[lax.rem(e, ring)])

    def w2_last(c):
        cols = pl.ds(c * width, width)
        return pltpu.make_async_copy(w2_hbm.at[n_exp - 1, :, cols], w2b.at[(n_exp - 1) % ring, :, cols], w2l_sem.at[c])

    for e in range(ring):
        w1_copy(e).start(priority=1)
        w2_copy(e).start(priority=1)

    def x_send(slot, piece, rel, to, k):
        return pltpu.make_async_remote_copy(src_ref=x_block(slot, piece), dst_ref=x_block(slot_of[rel], piece),
                                            send_sem=sx_sem.at[k, piece], recv_sem=rx_sem.at[rel, piece],
                                            device_id={"seq": to}, device_id_type=MESH)

    x_sends = []

    def x_start(slot, piece, rel, to, k):
        copy = x_send(slot, piece, rel, to, k)
        copy.start()
        x_sends.append(copy)

    pl.semaphore_wait(barrier, 3)
    own_x(0).wait()
    x_start(0, 0, 1, xnb, 1)
    own_x(2).wait()
    x_start(0, 2, 2, ynb, 2)
    own_x(1).wait()
    x_start(0, 1, 1, xnb, 1)
    own_x(3).wait()
    x_start(0, 3, 2, ynb, 2)
    for piece in (0, 1):
        x_start(0, piece + 2, 1, xnb, 1)
        x_start(0, piece, 2, ynb, 2)
    for piece in range(4):
        x_start(0, piece, 0, part, 0)

    own_phi.wait()
    for c in range(n_slots // 128):
        cols = pl.ds(c * 128, 128)
        p32 = phi_v[:, cols].astype(F32)
        pn[:, cols] = (p32 * lax.rsqrt(jnp.sum(p32 * p32, axis=0, keepdims=True) + EPSILON)).astype(BF16)
    chip_cols = pl.ds(pl.multiple_of(chip * 128, 128), 128)
    pnt[...] = pn[:, chip_cols].T
    own_g.wait()
    own_len.wait()
    g = g_ref[0]

    def normalise(slot):
        for b in range(batch):
            xn[b, slot] = row_normed(xg[b, slot])

    normalise(0)
    for b in range(batch):
        own_l = g * jnp.dot(xn[b, 0], pn[...], preferred_element_type=F32)
        c_exp = jnp.exp(own_l - jnp.max(own_l, axis=1, keepdims=True))
        cw[b] = c_exp.astype(BF16)
        qs[b] = jnp.broadcast_to(jnp.sum(c_exp, axis=1, keepdims=True), qs.shape[1:])

    own_pnt = pnt[pl.ds(pl.multiple_of(core * slots, slots), slots), :]
    near_tok = 4 * tok

    def slot_logits(b, half):
        rows = xn[b, 4 * half:4 * half + 4].reshape(near_tok, d_model)
        lt = g * lax.dot_general(own_pnt, rows, (((1,), (1,)), ((), ())), preferred_element_type=F32)
        lane = lax.broadcasted_iota(jnp.int32, lt.shape, 1)
        pos = lane
        for n, slot in enumerate(range(4 * half, 4 * half + 4)):
            owner = me if slot == 0 else owners[slot_of.index(slot)]
            pos = jnp.where(lane >= n * tok, lane + (owner - n) * tok, pos)
        return jnp.where(pos < len_ref[b], lt, NEG_FILL)

    def x_wait(rel, piece):
        x_send(0, piece, rel, part, 0).wait_recv()

    for piece in (0, 1):
        x_wait(1, piece)
        x_start(2, piece, 3, ynb, 3)
        x_start(2, piece, 4, part, 4)
        x_wait(2, piece + 2)
        x_start(3, piece + 2, 3, xnb, 3)
        x_start(3, piece + 2, 5, part, 5)
    for piece in range(4):
        x_wait(0, piece)
    normalise(1)
    for piece in (0, 1):
        x_wait(1, piece + 2)
        x_start(2, piece + 2, 4, part, 4)
        x_wait(2, piece)
        x_start(3, piece, 5, part, 5)
    normalise(2)
    normalise(3)
    for b in range(batch):
        la[b] = slot_logits(b, 0)
    for piece in (0, 2, 1, 3):
        x_wait(3, piece)
        x_start(6, piece, 6, part, 6)
    for rel in (4, 5):
        for piece in range(4):
            x_wait(rel, piece)
    for slot in (4, 5, 6):
        normalise(slot)
    for piece in range(4):
        x_wait(6, piece)
    normalise(7)
    for b in range(batch):
        near, far = la[b], slot_logits(b, 1)
        top = jnp.maximum(jnp.max(near, axis=1, keepdims=True), jnp.max(far, axis=1, keepdims=True))
        d_exp = jnp.concatenate([jnp.exp(near - top), jnp.exp(far - top)], axis=1)
        z = jnp.sum(d_exp, axis=1, keepdims=True)
        tokens = xg[b].reshape(2 * near_tok, d_model)
        slot_sum = jnp.dot(d_exp.astype(BF16), tokens, preferred_element_type=F32)
        xs[b] = (slot_sum / z).astype(BF16).astype(F32)

    def y_rows(dev, e):
        return pl.ds(pl.multiple_of(dev * slots + e * per, per), per)

    def y_send(owner, e, rel, to, recv, cols=slice(None)):
        block = yg.at[:, y_rows(owner, e), cols]
        return pltpu.make_async_remote_copy(src_ref=block, dst_ref=block, send_sem=sy_sem.at[rel], recv_sem=recv,
                                            device_id={"seq": to}, device_id_type=MESH)

    def y_chunk(owner, e, c, rel, to, recv):
        return y_send(owner, e, rel, to, recv, pl.ds(c * width, width))

    def send_own(e, cols, recvs):
        for rel, to in ((3, dia), (1, xnb), (2, ynb), (0, part)):
            y_send(me, e, rel, to, recvs.at[rel], cols).start()

    def y_wait(e, rel):
        y_send(last_owners[rel], e, rel, part, ry_sem.at[e, rel]).wait_recv()

    def forward(e):
        for rel in (1, 2, 3):
            y_wait(e, rel)
            y_send(last_owners[rel], e, rel + 3, part, ry_sem.at[e, rel + 3]).start()

    fblk = 1024

    def hidden(e, slot):
        rows = xs[:, pl.ds(pl.multiple_of(e * per, per), per), :].reshape(batch * per, d_model)
        for f in range(ff // fblk):
            cols = pl.ds(f * fblk, fblk)
            up = jnp.dot(rows, w1b[slot, :, cols], preferred_element_type=F32)
            h_v[:, cols] = jax.nn.gelu(up).astype(BF16).astype(F32)

    def outputs(e, slot, cols):
        out = jnp.dot(h_v[...], w2b[slot, :, cols], preferred_element_type=F32).astype(BF16)
        yg[:, y_rows(me, e), cols] = out.reshape(batch, per, cols.size)

    @pl.loop(0, n_exp - 1)
    def _(e):
        w1_copy(e).wait()
        w2_copy(e).wait()
        hidden(e, e)

        @pl.when(e == 0)
        def _():
            w1_copy(last).start(priority=1)

        for c in range(2):
            outputs(e, e, pl.ds(c * 2 * width, 2 * width))
            send_own(e, pl.ds(c * 2 * width, 2 * width), ry_sem.at[e])

        @pl.when(e == 0)
        def _():
            for c in range(chunks):
                w2_last(c).start(priority=1)

        @pl.when(e > 1)
        def _():
            forward(e - 2)

    w1_copy(last).wait()
    hidden(last, last % ring)
    for c in range(chunks):
        w2_last(c).wait()
        outputs(last, last % ring, pl.ds(c * width, width))
        send_own(last, pl.ds(c * width, width), rl_sem.at[c])
        if c == 0:
            forward(last - 2)
    forward(last - 1)
    for c in range(chunks):
        for rel in (1, 2, 3):
            y_chunk(last_owners[rel], last, c, rel, part, rl_sem.at[c, rel]).wait_recv()
            y_chunk(last_owners[rel], last, c, rel + 3, part, rl_sem.at[c, rel + 3]).start()
    for e in range(last):
        for rel in (0, 4, 5, 6):
            y_wait(e, rel)
    for c in range(chunks):
        for rel in (0, 4, 5, 6):
            y_chunk(last_owners[rel], last, c, rel, part, rl_sem.at[c, rel]).wait_recv()

    first = me * tok
    for b in range(batch):
        mixed = jnp.dot(cw[b], yg[b], preferred_element_type=F32) / qs[b][:, :1]
        pos = first + lax.broadcasted_iota(jnp.int32, mixed.shape, 0)
        y_ref[b] = jnp.where(pos < len_ref[b], mixed, 0.0).astype(BF16)

    for copy in x_sends:
        copy.wait_send()
    for rel in range(7):
        sent = yg.at[:, pl.ds(0, slots), :]
        pltpu.make_async_remote_copy(src_ref=sent, dst_ref=sent, send_sem=sy_sem.at[rel], recv_sem=ry_sem.at[0, rel],
                                     device_id={"seq": part}, device_id_type=MESH).wait_send()


def solution(mesh):
    seq_size = mesh.shape["seq"]

    def local_layer(tok_blk, len_blk, slot_param, logit_scale, w_in, w_out):
        batch, tok, d_model = tok_blk.shape
        n_slots = slot_param.shape[1]
        n_exp, _, ff = w_in.shape
        slots = n_slots // seq_size
        ring = n_exp - 1
        chunks = 4
        dma = pltpu.SemaphoreType.DMA
        sems = (dma, dma, dma((4,)), dma, dma((ring,)), dma((ring,)), dma((chunks,)),
                dma((7, 4)), dma((7, 4)), dma((7,)), dma((n_exp, 7)), dma((chunks, 7)))
        return pl.pallas_call(
            functools.partial(layer_kernel, sems),
            out_shape=pltpu.VMEM((batch, tok, d_model), BF16),
            in_specs=[pl.BlockSpec(memory_space=pltpu.HBM)] * 6,
            out_specs=pl.BlockSpec(memory_space=pltpu.VMEM),
            scratch_shapes=[
                pltpu.VMEM((batch, seq_size, tok, d_model), BF16),
                pltpu.VMEM((batch, seq_size, tok, d_model), BF16),
                pltpu.VMEM((batch, slots, tok * seq_size // 2), F32),
                pltpu.VMEM((d_model, n_slots), BF16),
                pltpu.VMEM((d_model, n_slots), BF16),
                pltpu.VMEM((2 * slots, d_model), BF16),
                pltpu.VMEM((batch, slots, d_model), F32),
                pltpu.VMEM((batch * slots // n_exp, ff), F32),
                pltpu.VMEM((batch, n_slots, d_model), BF16),
                pltpu.VMEM((batch, tok, n_slots), BF16),
                pltpu.VMEM((batch, tok, 128), F32),
                pltpu.VMEM((ring, d_model, ff), BF16),
                pltpu.VMEM((ring, ff, d_model), BF16),
                pltpu.SMEM((batch,), jnp.int32),
                pltpu.SMEM((1,), F32),
            ],
            compiler_params=pltpu.CompilerParams(collective_id=0, has_side_effects=True, vmem_limit_bytes=60 * 1024 * 1024),
        )(len_blk, logit_scale.reshape(1), tok_blk, slot_param, w_in, w_out)

    return jax.shard_map(local_layer, mesh=mesh, in_specs=(P("data", "seq", None), P("data"), P(None, None), P(), P("seq", None, None), P("seq", None, None)), out_specs=P("data", "seq", None), check_vma=False)
```

```python
import functools

import jax
import jax.numpy as jnp
from jax import lax
from jax.experimental import pallas as pl
from jax.experimental.pallas import tpu as pltpu
from jax.sharding import PartitionSpec as P

EPSILON = 1e-6
NEG_FILL = -1e30
MESH = pl.DeviceIdType.MESH
F32 = jnp.float32
BF16 = jnp.bfloat16


def row_normed(v):
    v32 = v.astype(F32)
    return (v32 * lax.rsqrt(jnp.sum(v32 * v32, axis=-1, keepdims=True) + EPSILON)).astype(BF16)


def layer_kernel(sems, *refs):
    pl.run_scoped(lambda *scoped: layer_body(*refs, *scoped), *sems)


def layer_body(len_hbm, g_hbm, x_hbm, phi_hbm, w1_hbm, w2_hbm, y_ref,
                 xg, xn, la, phi_v, pn, pnt, xs, h_v, yg, cw, qs, w1b, w2b, len_ref, g_ref,
                 len_sem, g_sem, x_sem, phi_sem, w1_sem, w2_sem, w2l_sem,
                 sx_sem, rx_sem, sy_sem, ry_sem, rl_sem):
    batch, tok, d_model = y_ref.shape
    n_exp = w1_hbm.shape[0]
    ff = w1_hbm.shape[2]
    n_slots = phi_hbm.shape[1]
    slots = xs.shape[1]
    per = slots // n_exp
    ring = w1b.shape[0]
    chunks = w2l_sem.shape[0]
    width = d_model // chunks
    last = n_exp - 1

    me = lax.axis_index("seq")
    core = lax.rem(me, 2)
    chip = lax.div(me, 2)
    part = me + 1 - 2 * core
    xsame = me + 2 - 4 * lax.rem(chip, 2)
    ysame = me + 4 - 8 * lax.div(chip, 2)
    dsame = xsame + ysame - me
    flip = 1 - 2 * core
    xnb, ynb, dia = xsame + flip, ysame + flip, dsame + flip
    owners = (part, xnb, ynb, dsame, xsame, ysame, dia)
    last_owners = (part, xnb, ynb, dia, xsame, ysame, dsame)

    barrier = pltpu.get_barrier_semaphore()
    for dev in owners[:3]:
        pl.semaphore_signal(barrier, inc=1, device_id={"seq": dev}, device_id_type=MESH)

    quarter = tok // 2
    slot_of = (1, 2, 3, 6, 4, 5, 7)

    def x_block(slot, piece):
        return xg.at[piece % 2, slot, pl.ds((piece // 2) * quarter, quarter), :]

    def own_x(piece):
        rows = pl.ds((piece // 2) * quarter, quarter)
        return pltpu.make_async_copy(x_hbm.at[piece % 2, rows, :], x_block(0, piece), x_sem.at[piece])

    for piece in (0, 2, 1, 3):
        own_x(piece).start()
    own_phi = pltpu.make_async_copy(phi_hbm, phi_v, phi_sem)
    own_phi.start()
    own_len = pltpu.make_async_copy(len_hbm, len_ref, len_sem)
    own_len.start()
    own_g = pltpu.make_async_copy(g_hbm, g_ref, g_sem)
    own_g.start()

    def w1_copy(e):
        return pltpu.make_async_copy(w1_hbm.at[e], w1b.at[lax.rem(e, ring)], w1_sem.at[lax.rem(e, ring)])

    def w2_copy(e):
        return pltpu.make_async_copy(w2_hbm.at[e], w2b.at[lax.rem(e, ring)], w2_sem.at[lax.rem(e, ring)])

    def w2_last(c):
        cols = pl.ds(c * width, width)
        return pltpu.make_async_copy(w2_hbm.at[n_exp - 1, :, cols], w2b.at[(n_exp - 1) % ring, :, cols], w2l_sem.at[c])

    for e in range(ring):
        w1_copy(e).start(priority=1)
        w2_copy(e).start(priority=1)

    def x_send(slot, piece, rel, to, k):
        return pltpu.make_async_remote_copy(src_ref=x_block(slot, piece), dst_ref=x_block(slot_of[rel], piece),
                                            send_sem=sx_sem.at[k, piece], recv_sem=rx_sem.at[rel, piece],
                                            device_id={"seq": to}, device_id_type=MESH)

    x_sends = []

    def x_start(slot, piece, rel, to, k):
        copy = x_send(slot, piece, rel, to, k)
        copy.start()
        x_sends.append(copy)

    pl.semaphore_wait(barrier, 3)
    own_x(0).wait()
    x_start(0, 0, 1, xnb, 1)
    own_x(2).wait()
    x_start(0, 2, 2, ynb, 2)
    own_x(1).wait()
    x_start(0, 1, 1, xnb, 1)
    own_x(3).wait()
    x_start(0, 3, 2, ynb, 2)
    for piece in (0, 1):
        x_start(0, piece + 2, 1, xnb, 1)
        x_start(0, piece, 2, ynb, 2)
    for piece in range(4):
        x_start(0, piece, 0, part, 0)

    own_phi.wait()
    for c in range(n_slots // 128):
        cols = pl.ds(c * 128, 128)
        p32 = phi_v[:, cols].astype(F32)
        pn[:, cols] = (p32 * lax.rsqrt(jnp.sum(p32 * p32, axis=0, keepdims=True) + EPSILON)).astype(BF16)
    chip_cols = pl.ds(pl.multiple_of(chip * 128, 128), 128)
    pnt[...] = pn[:, chip_cols].T
    own_g.wait()
    own_len.wait()
    g = g_ref[0]

    def normalise(slot):
        for b in range(batch):
            xn[b, slot] = row_normed(xg[b, slot])

    normalise(0)
    for b in range(batch):
        own_l = g * jnp.dot(xn[b, 0], pn[...], preferred_element_type=F32)
        c_exp = jnp.exp(own_l - jnp.max(own_l, axis=1, keepdims=True))
        cw[b] = c_exp.astype(BF16)
        qs[b] = jnp.broadcast_to(jnp.sum(c_exp, axis=1, keepdims=True), qs.shape[1:])

    own_pnt = pnt[pl.ds(pl.multiple_of(core * slots, slots), slots), :]
    near_tok = 4 * tok

    def slot_logits(b, half):
        rows = xn[b, 4 * half:4 * half + 4].reshape(near_tok, d_model)
        lt = g * lax.dot_general(own_pnt, rows, (((1,), (1,)), ((), ())), preferred_element_type=F32)
        lane = lax.broadcasted_iota(jnp.int32, lt.shape, 1)
        pos = lane
        for n, slot in enumerate(range(4 * half, 4 * half + 4)):
            owner = me if slot == 0 else owners[slot_of.index(slot)]
            pos = jnp.where(lane >= n * tok, lane + (owner - n) * tok, pos)
        return jnp.where(pos < len_ref[b], lt, NEG_FILL)

    def x_wait(rel, piece):
        x_send(0, piece, rel, part, 0).wait_recv()

    for piece in (0, 1):
        x_wait(1, piece)
        x_start(2, piece, 3, ynb, 3)
        x_start(2, piece, 4, part, 4)
        x_wait(2, piece + 2)
        x_start(3, piece + 2, 3, xnb, 3)
        x_start(3, piece + 2, 5, part, 5)
    for piece in range(4):
        x_wait(0, piece)
    normalise(1)
    for piece in (0, 1):
        x_wait(1, piece + 2)
        x_start(2, piece + 2, 4, part, 4)
        x_wait(2, piece)
        x_start(3, piece, 5, part, 5)
    normalise(2)
    normalise(3)
    for b in range(batch):
        la[b] = slot_logits(b, 0)
    for piece in (0, 2, 1, 3):
        x_wait(3, piece)
        x_start(6, piece, 6, part, 6)
    for rel in (4, 5):
        for piece in range(4):
            x_wait(rel, piece)
    for slot in (4, 5, 6):
        normalise(slot)
    for b in range(batch):
        x_wait(6, b)
        x_wait(6, b + 2)
        xn[b, 7] = row_normed(xg[b, 7])
        near, far = la[b], slot_logits(b, 1)
        top = jnp.maximum(jnp.max(near, axis=1, keepdims=True), jnp.max(far, axis=1, keepdims=True))
        d_exp = jnp.concatenate([jnp.exp(near - top), jnp.exp(far - top)], axis=1)
        z = jnp.sum(d_exp, axis=1, keepdims=True)
        tokens = xg[b].reshape(2 * near_tok, d_model)
        slot_sum = jnp.dot(d_exp.astype(BF16), tokens, preferred_element_type=F32)
        xs[b] = (slot_sum / z).astype(BF16).astype(F32)

    def y_rows(dev, e):
        return pl.ds(pl.multiple_of(dev * slots + e * per, per), per)

    def y_send(owner, e, rel, to, recv, cols=slice(None)):
        block = yg.at[:, y_rows(owner, e), cols]
        return pltpu.make_async_remote_copy(src_ref=block, dst_ref=block, send_sem=sy_sem.at[rel], recv_sem=recv,
                                            device_id={"seq": to}, device_id_type=MESH)

    def y_chunk(owner, e, c, rel, to, recv):
        return y_send(owner, e, rel, to, recv, pl.ds(c * width, width))

    def send_own(e, cols, recvs):
        for rel, to in ((3, dia), (1, xnb), (2, ynb), (0, part)):
            y_send(me, e, rel, to, recvs.at[rel], cols).start()

    def y_wait(e, rel):
        y_send(last_owners[rel], e, rel, part, ry_sem.at[e, rel]).wait_recv()

    def forward(e):
        for rel in (1, 2, 3):
            y_wait(e, rel)
            y_send(last_owners[rel], e, rel + 3, part, ry_sem.at[e, rel + 3]).start()

    fblk = 1024

    def hidden(e, slot, negate_high=False):
        rows = xs[:, pl.ds(pl.multiple_of(e * per, per), per), :].reshape(batch * per, d_model)
        for f in range(ff // fblk):
            cols = pl.ds(f * fblk, fblk)
            up = jnp.dot(rows, w1b[slot, :, cols], preferred_element_type=F32)
            act = jax.nn.gelu(up).astype(BF16).astype(F32)
            h_v[:, cols] = -act if negate_high and f * fblk >= ff // 2 else act

    def outputs(e, slot, cols):
        if cols.size > width:
            out = jnp.dot(h_v[...], w2b[slot, :, cols], preferred_element_type=F32)
        else:
            low, high = pl.ds(0, ff // 2), pl.ds(ff // 2, ff // 2)
            out = (jnp.dot(h_v[:, low], w2b[slot, low, cols], preferred_element_type=F32)
                   - jnp.dot(h_v[:, high], w2b[slot, high, cols], preferred_element_type=F32))
        out = out.astype(BF16)
        yg[:, y_rows(me, e), cols] = out.reshape(batch, per, cols.size)

    @pl.loop(0, n_exp - 1)
    def _(e):
        w1_copy(e).wait()
        hidden(e, e)

        @pl.when(e == 0)
        def _():
            w1_copy(last).start(priority=1)

        w2_copy(e).wait()

        for c in range(2):
            outputs(e, e, pl.ds(c * 2 * width, 2 * width))
            send_own(e, pl.ds(c * 2 * width, 2 * width), ry_sem.at[e])

        @pl.when(e == 0)
        def _():
            for c in range(chunks):
                w2_last(c).start(priority=1)

        @pl.when(e > 1)
        def _():
            forward(e - 2)

    w1_copy(last).wait()
    hidden(last, last % ring, True)
    for c in range(chunks):
        w2_last(c).wait()
        outputs(last, last % ring, pl.ds(c * width, width))
        send_own(last, pl.ds(c * width, width), rl_sem.at[c])
        if c == 0:
            forward(last - 2)
    forward(last - 1)
    for c in range(chunks):
        for rel in (1, 2, 3):
            y_chunk(last_owners[rel], last, c, rel, part, rl_sem.at[c, rel]).wait_recv()
            y_chunk(last_owners[rel], last, c, rel + 3, part, rl_sem.at[c, rel + 3]).start()
    for e in range(last):
        for rel in (0, 4, 5, 6):
            y_wait(e, rel)
    first = me * tok
    for c in range(chunks):
        for rel in (0, 4, 5, 6):
            y_chunk(last_owners[rel], last, c, rel, part, rl_sem.at[c, rel]).wait_recv()
        cols = pl.ds(c * width, width)
        for b in range(batch):
            mixed = jnp.dot(cw[b], yg[b, :, cols], preferred_element_type=F32) / qs[b][:, :1]
            pos = first + lax.broadcasted_iota(jnp.int32, mixed.shape, 0)
            y_ref[b, :, cols] = jnp.where(pos < len_ref[b], mixed, 0.0).astype(BF16)

    for copy in x_sends:
        copy.wait_send()
    for rel in range(7):
        sent = yg.at[:, pl.ds(0, slots), :]
        pltpu.make_async_remote_copy(src_ref=sent, dst_ref=sent, send_sem=sy_sem.at[rel], recv_sem=ry_sem.at[0, rel],
                                     device_id={"seq": part}, device_id_type=MESH).wait_send()


def solution(mesh):
    seq_size = mesh.shape["seq"]

    def local_layer(tok_blk, len_blk, slot_param, logit_scale, w_in, w_out):
        batch, tok, d_model = tok_blk.shape
        n_slots = slot_param.shape[1]
        n_exp, _, ff = w_in.shape
        slots = n_slots // seq_size
        ring = n_exp - 1
        chunks = 4
        dma = pltpu.SemaphoreType.DMA
        sems = (dma, dma, dma((4,)), dma, dma((ring,)), dma((ring,)), dma((chunks,)),
                dma((7, 4)), dma((7, 4)), dma((7,)), dma((n_exp, 7)), dma((chunks, 7)))
        return pl.pallas_call(
            functools.partial(layer_kernel, sems),
            out_shape=pltpu.VMEM((batch, tok, d_model), BF16),
            in_specs=[pl.BlockSpec(memory_space=pltpu.HBM)] * 6,
            out_specs=pl.BlockSpec(memory_space=pltpu.VMEM),
            scratch_shapes=[
                pltpu.VMEM((batch, seq_size, tok, d_model), BF16),
                pltpu.VMEM((batch, seq_size, tok, d_model), BF16),
                pltpu.VMEM((batch, slots, tok * seq_size // 2), F32),
                pltpu.VMEM((d_model, n_slots), BF16),
                pltpu.VMEM((d_model, n_slots), BF16),
                pltpu.VMEM((2 * slots, d_model), BF16),
                pltpu.VMEM((batch, slots, d_model), F32),
                pltpu.VMEM((batch * slots // n_exp, ff), F32),
                pltpu.VMEM((batch, n_slots, d_model), BF16),
                pltpu.VMEM((batch, tok, n_slots), BF16),
                pltpu.VMEM((batch, tok, 128), F32),
                pltpu.VMEM((ring, d_model, ff), BF16),
                pltpu.VMEM((ring, ff, d_model), BF16),
                pltpu.SMEM((batch,), jnp.int32),
                pltpu.SMEM((1,), F32),
            ],
            compiler_params=pltpu.CompilerParams(collective_id=0, has_side_effects=True, vmem_limit_bytes=60 * 1024 * 1024),
        )(len_blk, logit_scale.reshape(1), tok_blk, slot_param, w_in, w_out)

    return jax.shard_map(local_layer, mesh=mesh, in_specs=(P("data", "seq", None), P("data"), P(None, None), P(), P("seq", None, None), P("seq", None, None)), out_specs=P("data", "seq", None), check_vma=False)
```

```python
import functools

import jax
import jax.numpy as jnp
from jax import lax
from jax.experimental import pallas as pl
from jax.experimental.pallas import tpu as pltpu
from jax.sharding import PartitionSpec as P

EPSILON = 1e-6
NEG_FILL = -1e30
MESH = pl.DeviceIdType.MESH
F32 = jnp.float32
BF16 = jnp.bfloat16


def row_normed(v):
    v32 = v.astype(F32)
    return (v32 * lax.rsqrt(jnp.sum(v32 * v32, axis=-1, keepdims=True) + EPSILON)).astype(BF16)


def layer_kernel(sems, *refs):
    pl.run_scoped(lambda *scoped: layer_body(*refs, *scoped), *sems)


def layer_body(len_hbm, g_hbm, x_hbm, phi_hbm, w1_hbm, w2_hbm, y_ref,
                 xg, xn, la, phi_v, pn, pnt, xs, h_v, yg, cw, qs, w1b, w2b, len_ref, g_ref,
                 len_sem, g_sem, x_sem, phi_sem, w1_sem, w1l_sem, w2_sem, w2l_sem,
                 sx_sem, rx_sem, sy_sem, ry_sem, rl_sem):
    batch, tok, d_model = y_ref.shape
    n_exp = w1_hbm.shape[0]
    ff = w1_hbm.shape[2]
    n_slots = phi_hbm.shape[1]
    slots = xs.shape[1]
    per = slots // n_exp
    ring = w1b.shape[0]
    chunks = w2l_sem.shape[0]
    width = d_model // chunks
    last = n_exp - 1

    me = lax.axis_index("seq")
    core = lax.rem(me, 2)
    chip = lax.div(me, 2)
    part = me + 1 - 2 * core
    xsame = me + 2 - 4 * lax.rem(chip, 2)
    ysame = me + 4 - 8 * lax.div(chip, 2)
    dsame = xsame + ysame - me
    flip = 1 - 2 * core
    xnb, ynb, dia = xsame + flip, ysame + flip, dsame + flip
    owners = (part, xnb, ynb, dsame, xsame, ysame, dia)
    last_owners = (part, xnb, ynb, dia, xsame, ysame, dsame)

    barrier = pltpu.get_barrier_semaphore()
    for dev in owners[:3]:
        pl.semaphore_signal(barrier, inc=1, device_id={"seq": dev}, device_id_type=MESH)

    quarter = tok // 2
    slot_of = (1, 2, 3, 6, 4, 5, 7)

    def x_block(slot, piece):
        return xg.at[piece % 2, slot, pl.ds((piece // 2) * quarter, quarter), :]

    def own_x(piece):
        rows = pl.ds((piece // 2) * quarter, quarter)
        return pltpu.make_async_copy(x_hbm.at[piece % 2, rows, :], x_block(0, piece), x_sem.at[piece])

    for piece in (0, 2, 1, 3):
        own_x(piece).start()
    own_phi = pltpu.make_async_copy(phi_hbm, phi_v, phi_sem)
    own_phi.start()
    own_len = pltpu.make_async_copy(len_hbm, len_ref, len_sem)
    own_len.start()
    own_g = pltpu.make_async_copy(g_hbm, g_ref, g_sem)
    own_g.start()

    def w1_copy(e):
        return pltpu.make_async_copy(w1_hbm.at[e], w1b.at[lax.rem(e, ring)], w1_sem.at[lax.rem(e, ring)])

    def w1_last(half):
        cols = pl.ds(half * (ff // 2), ff // 2)
        return pltpu.make_async_copy(w1_hbm.at[last, :, cols], w1b.at[last % ring, :, cols], w1l_sem.at[half])

    def w2_copy(e):
        return pltpu.make_async_copy(w2_hbm.at[e], w2b.at[lax.rem(e, ring)], w2_sem.at[lax.rem(e, ring)])

    def w2_last(c):
        cols = pl.ds(c * width, width)
        return pltpu.make_async_copy(w2_hbm.at[n_exp - 1, :, cols], w2b.at[(n_exp - 1) % ring, :, cols], w2l_sem.at[c])

    for e in range(ring):
        w1_copy(e).start(priority=1)
        w2_copy(e).start(priority=1)

    def x_send(slot, piece, rel, to, k):
        return pltpu.make_async_remote_copy(src_ref=x_block(slot, piece), dst_ref=x_block(slot_of[rel], piece),
                                            send_sem=sx_sem.at[k, piece], recv_sem=rx_sem.at[rel, piece],
                                            device_id={"seq": to}, device_id_type=MESH)

    x_sends = []

    def x_start(slot, piece, rel, to, k):
        copy = x_send(slot, piece, rel, to, k)
        copy.start()
        x_sends.append(copy)

    pl.semaphore_wait(barrier, 3)
    own_x(0).wait()
    x_start(0, 0, 1, xnb, 1)
    own_x(2).wait()
    x_start(0, 2, 2, ynb, 2)
    own_x(1).wait()
    x_start(0, 1, 1, xnb, 1)
    own_x(3).wait()
    x_start(0, 3, 2, ynb, 2)
    for piece in (0, 1):
        x_start(0, piece + 2, 1, xnb, 1)
        x_start(0, piece, 2, ynb, 2)
    for piece in range(4):
        x_start(0, piece, 0, part, 0)

    own_phi.wait()
    for c in range(n_slots // 128):
        cols = pl.ds(c * 128, 128)
        p32 = phi_v[:, cols].astype(F32)
        pn[:, cols] = (p32 * lax.rsqrt(jnp.sum(p32 * p32, axis=0, keepdims=True) + EPSILON)).astype(BF16)
    chip_cols = pl.ds(pl.multiple_of(chip * 128, 128), 128)
    half_d = d_model // 2
    pnt[:, :half_d] = pn[:half_d, chip_cols].T
    pnt[:, half_d:] = -pn[half_d:, chip_cols].T
    own_g.wait()
    own_len.wait()
    g = g_ref[0]

    def normalise(slot):
        for b in range(batch):
            xn[b, slot] = row_normed(xg[b, slot])

    normalise(0)
    for b in range(batch):
        own_l = g * jnp.dot(xn[b, 0], pn[...], preferred_element_type=F32)
        c_exp = jnp.exp(own_l - jnp.max(own_l, axis=1, keepdims=True))
        cw[b] = c_exp.astype(BF16)
        qs[b] = jnp.broadcast_to(jnp.sum(c_exp, axis=1, keepdims=True), qs.shape[1:])

    own_pnt = pnt[pl.ds(pl.multiple_of(core * slots, slots), slots), :]
    near_tok = 4 * tok

    def slot_logits(b, half):
        rows = xn[b, 4 * half:4 * half + 4].reshape(near_tok, d_model)
        low, high = (lax.dot_general(own_pnt[:, d:d + half_d], rows[:, d:d + half_d], (((1,), (1,)), ((), ())),
                                     preferred_element_type=F32) for d in (0, half_d))
        lt = g * (low - high)
        lane = lax.broadcasted_iota(jnp.int32, lt.shape, 1)
        pos = lane
        for n, slot in enumerate(range(4 * half, 4 * half + 4)):
            owner = me if slot == 0 else owners[slot_of.index(slot)]
            pos = jnp.where(lane >= n * tok, lane + (owner - n) * tok, pos)
        return jnp.where(pos < len_ref[b], lt, NEG_FILL)

    def x_wait(rel, piece):
        x_send(0, piece, rel, part, 0).wait_recv()

    for piece in (0, 1):
        x_wait(1, piece)
        x_start(2, piece, 3, ynb, 3)
        x_start(2, piece, 4, part, 4)
        x_wait(2, piece + 2)
        x_start(3, piece + 2, 3, xnb, 3)
        x_start(3, piece + 2, 5, part, 5)
    for piece in range(4):
        x_wait(0, piece)
    normalise(1)
    for piece in (0, 1):
        x_wait(1, piece + 2)
        x_start(2, piece + 2, 4, part, 4)
        x_wait(2, piece)
        x_start(3, piece, 5, part, 5)
    normalise(2)
    normalise(3)
    for b in range(batch):
        la[b] = slot_logits(b, 0)
    for piece in (0, 2, 1, 3):
        x_wait(3, piece)
        x_start(6, piece, 6, part, 6)
    for rel in (4, 5):
        for piece in range(4):
            x_wait(rel, piece)
    for slot in (4, 5, 6):
        normalise(slot)
    for b in range(batch):
        x_wait(6, b)
        x_wait(6, b + 2)
        xn[b, 7] = row_normed(xg[b, 7])
        near, far = la[b], slot_logits(b, 1)
        top = jnp.maximum(jnp.max(near, axis=1, keepdims=True), jnp.max(far, axis=1, keepdims=True))
        d_exp = jnp.concatenate([jnp.exp(near - top), jnp.exp(far - top)], axis=1)
        z = jnp.sum(d_exp, axis=1, keepdims=True)
        tokens = xg[b].reshape(2 * near_tok, d_model)
        slot_sum = jnp.dot(d_exp.astype(BF16), tokens, preferred_element_type=F32)
        xs[b] = (slot_sum / z).astype(BF16).astype(F32)

    def y_rows(dev, e):
        return pl.ds(pl.multiple_of(dev * slots + e * per, per), per)

    def y_send(owner, e, rel, to, recv, cols=slice(None)):
        block = yg.at[:, y_rows(owner, e), cols]
        return pltpu.make_async_remote_copy(src_ref=block, dst_ref=block, send_sem=sy_sem.at[rel], recv_sem=recv,
                                            device_id={"seq": to}, device_id_type=MESH)

    def y_chunk(owner, e, c, rel, to, recv):
        return y_send(owner, e, rel, to, recv, pl.ds(c * width, width))

    def send_own(e, cols, recvs):
        for rel, to in ((3, dia), (1, xnb), (2, ynb), (0, part)):
            y_send(me, e, rel, to, recvs.at[rel], cols).start()

    def y_wait(e, rel):
        y_send(last_owners[rel], e, rel, part, ry_sem.at[e, rel]).wait_recv()

    def forward(e):
        for rel in (1, 2, 3):
            y_wait(e, rel)
            y_send(last_owners[rel], e, rel + 3, part, ry_sem.at[e, rel + 3]).start()

    fblk = 1024

    def hidden(e, slot, split=False):
        rows = xs[:, pl.ds(pl.multiple_of(e * per, per), per), :].reshape(batch * per, d_model)
        for f in range(ff // fblk):
            if split and f * fblk % (ff // 2) == 0:
                w1_last(2 * f * fblk // ff).wait()
            cols = pl.ds(f * fblk, fblk)
            up = jnp.dot(rows, w1b[slot, :, cols], preferred_element_type=F32)
            act = jax.nn.gelu(up).astype(BF16).astype(F32)
            h_v[:, cols] = -act if split and f * fblk >= ff // 2 else act

    def outputs(e, slot, cols):
        if cols.size > width:
            out = jnp.dot(h_v[...], w2b[slot, :, cols], preferred_element_type=F32)
        else:
            low, high = pl.ds(0, ff // 2), pl.ds(ff // 2, ff // 2)
            out = (jnp.dot(h_v[:, low], w2b[slot, low, cols], preferred_element_type=F32)
                   - jnp.dot(h_v[:, high], w2b[slot, high, cols], preferred_element_type=F32))
        out = out.astype(BF16)
        yg[:, y_rows(me, e), cols] = out.reshape(batch, per, cols.size)

    w1_copy(0).wait()
    hidden(0, 0)
    for half in (0, 1):
        w1_last(half).start(priority=1)
    w2_copy(0).wait()
    outputs(0, 0, pl.ds(0, d_model))
    send_own(0, pl.ds(0, d_model), ry_sem.at[0])
    for c in range(chunks):
        w2_last(c).start(priority=1)

    @pl.loop(1, last)
    def _(e):
        w1_copy(e).wait()
        hidden(e, e)
        w2_copy(e).wait()
        for c in range(2):
            outputs(e, e, pl.ds(c * 2 * width, 2 * width))
            send_own(e, pl.ds(c * 2 * width, 2 * width), ry_sem.at[e])

    forward(0)
    hidden(last, last % ring, True)
    for c in range(chunks):
        w2_last(c).wait()
        outputs(last, last % ring, pl.ds(c * width, width))
        send_own(last, pl.ds(c * width, width), rl_sem.at[c])
        if c == 1:
            for e in range(1, last - 1):
                forward(e)
    forward(last - 1)
    for c in range(chunks):
        for rel in (1, 2, 3):
            y_chunk(last_owners[rel], last, c, rel, part, rl_sem.at[c, rel]).wait_recv()
            y_chunk(last_owners[rel], last, c, rel + 3, part, rl_sem.at[c, rel + 3]).start()
    for e in range(last):
        for rel in (0, 4, 5, 6):
            y_wait(e, rel)
    def y_sent(rel):
        sent = yg.at[:, pl.ds(0, slots), :]
        pltpu.make_async_remote_copy(src_ref=sent, dst_ref=sent, send_sem=sy_sem.at[rel], recv_sem=ry_sem.at[0, rel],
                                     device_id={"seq": part}, device_id_type=MESH).wait_send()

    for copy in x_sends:
        copy.wait_send()
    for rel in range(4):
        y_sent(rel)
    first = me * tok
    for c in range(chunks):
        for rel in (0, 4, 5, 6):
            y_chunk(last_owners[rel], last, c, rel, part, rl_sem.at[c, rel]).wait_recv()
        cols = pl.ds(c * width, width)
        for b in range(batch):
            mixed = jnp.dot(cw[b], yg[b, :, cols], preferred_element_type=F32) / qs[b][:, :1]
            pos = first + lax.broadcasted_iota(jnp.int32, mixed.shape, 0)
            y_ref[b, :, cols] = jnp.where(pos < len_ref[b], mixed, 0.0).astype(BF16)

    for rel in (4, 5, 6):
        y_sent(rel)


def solution(mesh):
    seq_size = mesh.shape["seq"]

    def local_layer(tok_blk, len_blk, slot_param, logit_scale, w_in, w_out):
        batch, tok, d_model = tok_blk.shape
        n_slots = slot_param.shape[1]
        n_exp, _, ff = w_in.shape
        slots = n_slots // seq_size
        ring = n_exp - 1
        chunks = 4
        dma = pltpu.SemaphoreType.DMA
        sems = (dma, dma, dma((4,)), dma, dma((ring,)), dma((2,)), dma((ring,)), dma((chunks,)),
                dma((7, 4)), dma((7, 4)), dma((7,)), dma((n_exp, 7)), dma((chunks, 7)))
        return pl.pallas_call(
            functools.partial(layer_kernel, sems),
            out_shape=pltpu.VMEM((batch, tok, d_model), BF16),
            in_specs=[pl.BlockSpec(memory_space=pltpu.HBM)] * 6,
            out_specs=pl.BlockSpec(memory_space=pltpu.VMEM),
            scratch_shapes=[
                pltpu.VMEM((batch, seq_size, tok, d_model), BF16),
                pltpu.VMEM((batch, seq_size, tok, d_model), BF16),
                pltpu.VMEM((batch, slots, tok * seq_size // 2), F32),
                pltpu.VMEM((d_model, n_slots), BF16),
                pltpu.VMEM((d_model, n_slots), BF16),
                pltpu.VMEM((2 * slots, d_model), BF16),
                pltpu.VMEM((batch, slots, d_model), F32),
                pltpu.VMEM((batch * slots // n_exp, ff), F32),
                pltpu.VMEM((batch, n_slots, d_model), BF16),
                pltpu.VMEM((batch, tok, n_slots), BF16),
                pltpu.VMEM((batch, tok, 128), F32),
                pltpu.VMEM((ring, d_model, ff), BF16),
                pltpu.VMEM((ring, ff, d_model), BF16),
                pltpu.SMEM((batch,), jnp.int32),
                pltpu.SMEM((1,), F32),
            ],
            compiler_params=pltpu.CompilerParams(collective_id=0, has_side_effects=True, vmem_limit_bytes=60 * 1024 * 1024),
        )(len_blk, logit_scale.reshape(1), tok_blk, slot_param, w_in, w_out)

    return jax.shard_map(local_layer, mesh=mesh, in_specs=(P("data", "seq", None), P("data"), P(None, None), P(), P("seq", None, None), P("seq", None, None)), out_specs=P("data", "seq", None), check_vma=False)
```

```python
import functools

import jax
import jax.numpy as jnp
from jax import lax
from jax.experimental import pallas as pl
from jax.experimental.pallas import tpu as pltpu
from jax.sharding import PartitionSpec as P

EPSILON = 1e-6
NEG_FILL = -1e30
MESH = pl.DeviceIdType.MESH
F32 = jnp.float32
BF16 = jnp.bfloat16


def row_normed(v):
    v32 = v.astype(F32)
    return (v32 * lax.rsqrt(jnp.sum(v32 * v32, axis=-1, keepdims=True) + EPSILON)).astype(BF16)


def layer_kernel(sems, *refs):
    pl.run_scoped(lambda *scoped: layer_body(*refs, *scoped), *sems)


def layer_body(len_hbm, g_hbm, x_hbm, phi_hbm, w1_hbm, w2_hbm, y_ref,
                 xg, xn, la, phi_v, pn, pnt, xs, h_v, yg, cw, qs, w1b, w2b, len_ref, g_ref,
                 len_sem, g_sem, x_sem, phi_sem, w1_sem, w1l_sem, w2_sem, w2l_sem,
                 sx_sem, rx_sem, sy_sem, ry_sem, rl_sem):
    batch, tok, d_model = y_ref.shape
    n_exp = w1_hbm.shape[0]
    ff = w1_hbm.shape[2]
    n_slots = phi_hbm.shape[1]
    slots = xs.shape[1]
    per = slots // n_exp
    ring = w1b.shape[0]
    chunks = w2l_sem.shape[0]
    width = d_model // chunks
    last = n_exp - 1

    me = lax.axis_index("seq")
    core = lax.rem(me, 2)
    chip = lax.div(me, 2)
    part = me + 1 - 2 * core
    xsame = me + 2 - 4 * lax.rem(chip, 2)
    ysame = me + 4 - 8 * lax.div(chip, 2)
    dsame = xsame + ysame - me
    flip = 1 - 2 * core
    xnb, ynb, dia = xsame + flip, ysame + flip, dsame + flip
    owners = (part, xnb, ynb, dsame, xsame, ysame, dia)
    last_owners = (part, xnb, ynb, dia, xsame, ysame, dsame)

    barrier = pltpu.get_barrier_semaphore()
    for dev in owners[:3]:
        pl.semaphore_signal(barrier, inc=1, device_id={"seq": dev}, device_id_type=MESH)

    quarter = tok // 2
    slot_of = (1, 2, 3, 6, 4, 5, 7)

    def x_block(slot, piece):
        return xg.at[piece % 2, slot, pl.ds((piece // 2) * quarter, quarter), :]

    def own_x(piece):
        rows = pl.ds((piece // 2) * quarter, quarter)
        return pltpu.make_async_copy(x_hbm.at[piece % 2, rows, :], x_block(0, piece), x_sem.at[piece])

    for piece in (0, 2, 1, 3):
        own_x(piece).start()
    own_phi = pltpu.make_async_copy(phi_hbm, phi_v, phi_sem)
    own_phi.start()
    own_len = pltpu.make_async_copy(len_hbm, len_ref, len_sem)
    own_len.start()
    own_g = pltpu.make_async_copy(g_hbm, g_ref, g_sem)
    own_g.start()

    def w1_copy(e):
        return pltpu.make_async_copy(w1_hbm.at[e], w1b.at[lax.rem(e, ring)], w1_sem.at[lax.rem(e, ring)])

    def w1_last(half):
        cols = pl.ds(half * (ff // 2), ff // 2)
        return pltpu.make_async_copy(w1_hbm.at[last, :, cols], w1b.at[last % ring, :, cols], w1l_sem.at[half])

    def w2_copy(e):
        return pltpu.make_async_copy(w2_hbm.at[e], w2b.at[lax.rem(e, ring)], w2_sem.at[lax.rem(e, ring)])

    def w2_last(c):
        cols = pl.ds(c * width, width)
        return pltpu.make_async_copy(w2_hbm.at[n_exp - 1, :, cols], w2b.at[(n_exp - 1) % ring, :, cols], w2l_sem.at[c])

    for e in range(ring):
        w1_copy(e).start(priority=1)
        w2_copy(e).start(priority=1)

    def x_send(slot, piece, rel, to, k):
        return pltpu.make_async_remote_copy(src_ref=x_block(slot, piece), dst_ref=x_block(slot_of[rel], piece),
                                            send_sem=sx_sem.at[k, piece], recv_sem=rx_sem.at[rel, piece],
                                            device_id={"seq": to}, device_id_type=MESH)

    x_sends = []

    def x_start(slot, piece, rel, to, k):
        copy = x_send(slot, piece, rel, to, k)
        copy.start()
        x_sends.append(copy)

    pl.semaphore_wait(barrier, 3)
    own_x(0).wait()
    x_start(0, 0, 1, xnb, 1)
    own_x(2).wait()
    x_start(0, 2, 2, ynb, 2)
    own_x(1).wait()
    x_start(0, 1, 1, xnb, 1)
    own_x(3).wait()
    x_start(0, 3, 2, ynb, 2)
    for piece in (0, 1):
        x_start(0, piece + 2, 1, xnb, 1)
        x_start(0, piece, 2, ynb, 2)
    for piece in range(4):
        x_start(0, piece, 0, part, 0)

    own_phi.wait()
    for c in range(n_slots // 128):
        cols = pl.ds(c * 128, 128)
        p32 = phi_v[:, cols].astype(F32)
        pn[:, cols] = (p32 * lax.rsqrt(jnp.sum(p32 * p32, axis=0, keepdims=True) + EPSILON)).astype(BF16)
    chip_cols = pl.ds(pl.multiple_of(chip * 128, 128), 128)
    half_d = d_model // 2
    pnt[:, :half_d] = pn[:half_d, chip_cols].T
    pnt[:, half_d:] = -pn[half_d:, chip_cols].T
    own_g.wait()
    own_len.wait()
    g = g_ref[0]

    def normalise(slot):
        for b in range(batch):
            xn[b, slot] = row_normed(xg[b, slot])

    normalise(0)
    for b in range(batch):
        own_l = g * jnp.dot(xn[b, 0], pn[...], preferred_element_type=F32)
        c_exp = jnp.exp(own_l - jnp.max(own_l, axis=1, keepdims=True))
        cw[b] = c_exp.astype(BF16)
        qs[b] = jnp.broadcast_to(jnp.sum(c_exp, axis=1, keepdims=True), qs.shape[1:])

    own_pnt = pnt[pl.ds(pl.multiple_of(core * slots, slots), slots), :]
    near_tok = 4 * tok

    def slot_logits(b, half):
        rows = xn[b, 4 * half:4 * half + 4].reshape(near_tok, d_model)
        low, high = (lax.dot_general(own_pnt[:, d:d + half_d], rows[:, d:d + half_d], (((1,), (1,)), ((), ())),
                                     preferred_element_type=F32) for d in (0, half_d))
        lt = g * (low - high)
        lane = lax.broadcasted_iota(jnp.int32, lt.shape, 1)
        pos = lane
        for n, slot in enumerate(range(4 * half, 4 * half + 4)):
            owner = me if slot == 0 else owners[slot_of.index(slot)]
            pos = jnp.where(lane >= n * tok, lane + (owner - n) * tok, pos)
        return jnp.where(pos < len_ref[b], lt, NEG_FILL)

    def x_wait(rel, piece):
        x_send(0, piece, rel, part, 0).wait_recv()

    for piece in (0, 1):
        x_wait(1, piece)
        x_start(2, piece, 3, ynb, 3)
        if piece == 1:
            x_start(2, piece, 6, ysame, 6)
        x_start(2, piece, 4, part, 4)
        x_wait(2, piece + 2)
        x_start(3, piece + 2, 3, xnb, 3)
        if piece == 1:
            x_start(3, piece + 2, 6, xsame, 6)
        x_start(3, piece + 2, 5, part, 5)
    for piece in range(4):
        x_wait(0, piece)
    normalise(1)
    for piece in (0, 1):
        x_wait(1, piece + 2)
        x_start(2, piece + 2, 4, part, 4)
        x_wait(2, piece)
        x_start(3, piece, 5, part, 5)
    normalise(2)
    normalise(3)
    for b in range(batch):
        la[b] = slot_logits(b, 0)
    for piece in (0, 2, 1, 3):
        x_wait(3, piece)
        if piece % 2 == 0:
            x_start(6, piece, 6, part, 6)
    for rel in (4, 5):
        for piece in range(4):
            x_wait(rel, piece)
    for slot in (4, 5, 6):
        normalise(slot)
    for piece in range(4):
        x_wait(6, piece)
    for b in range(batch):
        xn[b, 7] = row_normed(xg[b, 7])
        near, far = la[b], slot_logits(b, 1)
        top = jnp.maximum(jnp.max(near, axis=1, keepdims=True), jnp.max(far, axis=1, keepdims=True))
        d_exp = jnp.concatenate([jnp.exp(near - top), jnp.exp(far - top)], axis=1)
        z = jnp.sum(d_exp, axis=1, keepdims=True)
        tokens = xg[b].reshape(2 * near_tok, d_model)
        slot_sum = jnp.dot(d_exp.astype(BF16), tokens, preferred_element_type=F32)
        xs[b] = (slot_sum / z).astype(BF16).astype(F32)

    def y_rows(dev, e):
        return pl.ds(pl.multiple_of(dev * slots + e * per, per), per)

    def y_send(owner, e, rel, to, recv, cols=slice(None)):
        block = yg.at[:, y_rows(owner, e), cols]
        return pltpu.make_async_remote_copy(src_ref=block, dst_ref=block, send_sem=sy_sem.at[rel], recv_sem=recv,
                                            device_id={"seq": to}, device_id_type=MESH)

    def y_chunk(owner, e, c, rel, to, recv):
        return y_send(owner, e, rel, to, recv, pl.ds(c * width, width))

    def send_own(e, cols, recvs):
        for rel, to in ((3, dia), (1, xnb), (2, ynb), (0, part)):
            y_send(me, e, rel, to, recvs.at[rel], cols).start()

    def y_wait(e, rel):
        y_send(last_owners[rel], e, rel, part, ry_sem.at[e, rel]).wait_recv()

    def forward(e):
        for rel in (1, 2, 3):
            y_wait(e, rel)
            y_send(last_owners[rel], e, rel + 3, part, ry_sem.at[e, rel + 3]).start()

    fblk = 1024

    def hidden(e, slot, split=False):
        rows = xs[:, pl.ds(pl.multiple_of(e * per, per), per), :].reshape(batch * per, d_model)
        for f in range(ff // fblk):
            if split and f * fblk % (ff // 2) == 0:
                w1_last(2 * f * fblk // ff).wait()
            cols = pl.ds(f * fblk, fblk)
            up = jnp.dot(rows, w1b[slot, :, cols], preferred_element_type=F32)
            act = jax.nn.gelu(up).astype(BF16).astype(F32)
            h_v[:, cols] = -act if split and f * fblk >= ff // 2 else act

    def outputs(e, slot, cols):
        if cols.size > width:
            out = jnp.dot(h_v[...], w2b[slot, :, cols], preferred_element_type=F32)
        else:
            low, high = pl.ds(0, ff // 2), pl.ds(ff // 2, ff // 2)
            out = (jnp.dot(h_v[:, low], w2b[slot, low, cols], preferred_element_type=F32)
                   - jnp.dot(h_v[:, high], w2b[slot, high, cols], preferred_element_type=F32))
        out = out.astype(BF16)
        yg[:, y_rows(me, e), cols] = out.reshape(batch, per, cols.size)

    w1_copy(0).wait()
    hidden(0, 0)
    for half in (0, 1):
        w1_last(half).start(priority=1)
    w2_copy(0).wait()
    outputs(0, 0, pl.ds(0, d_model))
    send_own(0, pl.ds(0, d_model), ry_sem.at[0])
    for c in range(chunks):
        w2_last(c).start(priority=1)

    @pl.loop(1, last)
    def _(e):
        w1_copy(e).wait()
        hidden(e, e)
        w2_copy(e).wait()
        for c in range(2):
            outputs(e, e, pl.ds(c * 2 * width, 2 * width))
            send_own(e, pl.ds(c * 2 * width, 2 * width), ry_sem.at[e])

    forward(0)
    hidden(last, last % ring, True)
    for c in range(chunks):
        w2_last(c).wait()
        outputs(last, last % ring, pl.ds(c * width, width))
        send_own(last, pl.ds(c * width, width), rl_sem.at[c])
        if c == 1:
            for e in range(1, last - 1):
                forward(e)
    forward(last - 1)
    for c in range(chunks):
        for rel in (1, 2, 3):
            y_chunk(last_owners[rel], last, c, rel, part, rl_sem.at[c, rel]).wait_recv()
            y_chunk(last_owners[rel], last, c, rel + 3, part, rl_sem.at[c, rel + 3]).start()
    for e in range(last):
        for rel in (0, 4, 5, 6):
            y_wait(e, rel)
    def y_sent(rel):
        sent = yg.at[:, pl.ds(0, slots), :]
        pltpu.make_async_remote_copy(src_ref=sent, dst_ref=sent, send_sem=sy_sem.at[rel], recv_sem=ry_sem.at[0, rel],
                                     device_id={"seq": part}, device_id_type=MESH).wait_send()

    for copy in x_sends:
        copy.wait_send()
    for rel in range(4):
        y_sent(rel)
    first = me * tok
    for c in range(chunks):
        for rel in (0, 4, 5, 6):
            y_chunk(last_owners[rel], last, c, rel, part, rl_sem.at[c, rel]).wait_recv()
        cols = pl.ds(c * width, width)
        for b in range(batch):
            mixed = jnp.dot(cw[b], yg[b, :, cols], preferred_element_type=F32) / qs[b][:, :1]
            pos = first + lax.broadcasted_iota(jnp.int32, mixed.shape, 0)
            y_ref[b, :, cols] = jnp.where(pos < len_ref[b], mixed, 0.0).astype(BF16)

    for rel in (4, 5, 6):
        y_sent(rel)


def solution(mesh):
    seq_size = mesh.shape["seq"]

    def local_layer(tok_blk, len_blk, slot_param, logit_scale, w_in, w_out):
        batch, tok, d_model = tok_blk.shape
        n_slots = slot_param.shape[1]
        n_exp, _, ff = w_in.shape
        slots = n_slots // seq_size
        ring = n_exp - 1
        chunks = 4
        dma = pltpu.SemaphoreType.DMA
        sems = (dma, dma, dma((4,)), dma, dma((ring,)), dma((2,)), dma((ring,)), dma((chunks,)),
                dma((7, 4)), dma((7, 4)), dma((7,)), dma((n_exp, 7)), dma((chunks, 7)))
        return pl.pallas_call(
            functools.partial(layer_kernel, sems),
            out_shape=pltpu.VMEM((batch, tok, d_model), BF16),
            in_specs=[pl.BlockSpec(memory_space=pltpu.HBM)] * 6,
            out_specs=pl.BlockSpec(memory_space=pltpu.VMEM),
            scratch_shapes=[
                pltpu.VMEM((batch, seq_size, tok, d_model), BF16),
                pltpu.VMEM((batch, seq_size, tok, d_model), BF16),
                pltpu.VMEM((batch, slots, tok * seq_size // 2), F32),
                pltpu.VMEM((d_model, n_slots), BF16),
                pltpu.VMEM((d_model, n_slots), BF16),
                pltpu.VMEM((2 * slots, d_model), BF16),
                pltpu.VMEM((batch, slots, d_model), F32),
                pltpu.VMEM((batch * slots // n_exp, ff), F32),
                pltpu.VMEM((batch, n_slots, d_model), BF16),
                pltpu.VMEM((batch, tok, n_slots), BF16),
                pltpu.VMEM((batch, tok, 128), F32),
                pltpu.VMEM((ring, d_model, ff), BF16),
                pltpu.VMEM((ring, ff, d_model), BF16),
                pltpu.SMEM((batch,), jnp.int32),
                pltpu.SMEM((1,), F32),
            ],
            compiler_params=pltpu.CompilerParams(collective_id=0, has_side_effects=True, vmem_limit_bytes=60 * 1024 * 1024),
        )(len_blk, logit_scale.reshape(1), tok_blk, slot_param, w_in, w_out)

    return jax.shard_map(local_layer, mesh=mesh, in_specs=(P("data", "seq", None), P("data"), P(None, None), P(), P("seq", None, None), P("seq", None, None)), out_specs=P("data", "seq", None), check_vma=False)
```

```python
import functools

import jax
import jax.numpy as jnp
from jax import lax
from jax.experimental import pallas as pl
from jax.experimental.pallas import tpu as pltpu
from jax.sharding import PartitionSpec as P

EPSILON = 1e-6
NEG_FILL = -1e30
MESH = pl.DeviceIdType.MESH
F32 = jnp.float32
BF16 = jnp.bfloat16


def row_normed(v):
    v32 = v.astype(F32)
    return (v32 * lax.rsqrt(jnp.sum(v32 * v32, axis=-1, keepdims=True) + EPSILON)).astype(BF16)


def layer_kernel(sems, *refs):
    pl.run_scoped(lambda *scoped: layer_body(*refs, *scoped), *sems)


def layer_body(len_hbm, g_hbm, x_hbm, phi_hbm, w1_hbm, w2_hbm, y_ref,
                 xg, xn, la, phi_v, pn, pnt, xs, h_v, yg, cw, qs, w1b, w2b, len_ref, g_ref,
                 len_sem, g_sem, x_sem, phi_sem, w1_sem, w1l_sem, w2_sem, w2l_sem,
                 sx_sem, rx_sem, sy_sem, ry_sem, rl_sem):
    batch, tok, d_model = y_ref.shape
    n_exp = w1_hbm.shape[0]
    ff = w1_hbm.shape[2]
    n_slots = phi_hbm.shape[1]
    slots = xs.shape[1]
    per = slots // n_exp
    ring = w1b.shape[0]
    chunks = w2l_sem.shape[0]
    width = d_model // chunks
    last = n_exp - 1

    me = lax.axis_index("seq")
    core = lax.rem(me, 2)
    chip = lax.div(me, 2)
    part = me + 1 - 2 * core
    xsame = me + 2 - 4 * lax.rem(chip, 2)
    ysame = me + 4 - 8 * lax.div(chip, 2)
    dsame = xsame + ysame - me
    flip = 1 - 2 * core
    xnb, ynb, dia = xsame + flip, ysame + flip, dsame + flip
    owners = (part, xnb, ynb, dsame, xsame, ysame, dia)
    last_owners = (part, xnb, ynb, dia, xsame, ysame, dsame)

    barrier = pltpu.get_barrier_semaphore()
    for dev in owners[:3]:
        pl.semaphore_signal(barrier, inc=1, device_id={"seq": dev}, device_id_type=MESH)

    quarter = tok // 2
    slot_of = (1, 2, 3, 6, 4, 5, 7)

    def x_block(slot, piece):
        return xg.at[piece % 2, slot, pl.ds((piece // 2) * quarter, quarter), :]

    def own_x(piece):
        rows = pl.ds((piece // 2) * quarter, quarter)
        return pltpu.make_async_copy(x_hbm.at[piece % 2, rows, :], x_block(0, piece), x_sem.at[piece])

    for piece in (0, 2, 1, 3):
        own_x(piece).start()
    own_phi = pltpu.make_async_copy(phi_hbm, phi_v, phi_sem)
    own_phi.start()
    own_len = pltpu.make_async_copy(len_hbm, len_ref, len_sem)
    own_len.start()
    own_g = pltpu.make_async_copy(g_hbm, g_ref, g_sem)
    own_g.start()

    def w1_copy(e):
        return pltpu.make_async_copy(w1_hbm.at[e], w1b.at[lax.rem(e, ring)], w1_sem.at[lax.rem(e, ring)])

    def w1_last(half):
        cols = pl.ds(half * (ff // 2), ff // 2)
        return pltpu.make_async_copy(w1_hbm.at[last, :, cols], w1b.at[last % ring, :, cols], w1l_sem.at[half])

    def w2_copy(e):
        return pltpu.make_async_copy(w2_hbm.at[e], w2b.at[lax.rem(e, ring)], w2_sem.at[lax.rem(e, ring)])

    def w2_last(c):
        cols = pl.ds(c * width, width)
        return pltpu.make_async_copy(w2_hbm.at[n_exp - 1, :, cols], w2b.at[(n_exp - 1) % ring, :, cols], w2l_sem.at[c])

    for e in range(ring):
        w1_copy(e).start(priority=1)
        w2_copy(e).start(priority=1)

    def x_send(slot, piece, rel, to, k):
        return pltpu.make_async_remote_copy(src_ref=x_block(slot, piece), dst_ref=x_block(slot_of[rel], piece),
                                            send_sem=sx_sem.at[k, piece], recv_sem=rx_sem.at[rel, piece],
                                            device_id={"seq": to}, device_id_type=MESH)

    x_sends = []

    def x_start(slot, piece, rel, to, k):
        copy = x_send(slot, piece, rel, to, k)
        copy.start()
        x_sends.append(copy)

    pl.semaphore_wait(barrier, 3)
    own_x(0).wait()
    x_start(0, 0, 1, xnb, 1)
    own_x(2).wait()
    x_start(0, 2, 2, ynb, 2)
    own_x(1).wait()
    x_start(0, 1, 1, xnb, 1)
    own_x(3).wait()
    x_start(0, 3, 2, ynb, 2)
    for piece in (0, 1):
        x_start(0, piece + 2, 1, xnb, 1)
        x_start(0, piece, 2, ynb, 2)

    own_phi.wait()
    for c in range(n_slots // 128):
        cols = pl.ds(c * 128, 128)
        p32 = phi_v[:, cols].astype(F32)
        pn[:, cols] = (p32 * lax.rsqrt(jnp.sum(p32 * p32, axis=0, keepdims=True) + EPSILON)).astype(BF16)
    chip_cols = pl.ds(pl.multiple_of(chip * 128, 128), 128)
    half_d = d_model // 2
    pnt[:, :half_d] = pn[:half_d, chip_cols].T
    pnt[:, half_d:] = -pn[half_d:, chip_cols].T
    own_g.wait()
    own_len.wait()
    g = g_ref[0]

    def normalise(slot):
        for b in range(batch):
            xn[b, slot] = row_normed(xg[b, slot])

    normalise(0)
    for b in range(batch):
        own_l = g * jnp.dot(xn[b, 0], pn[...], preferred_element_type=F32)
        c_exp = jnp.exp(own_l - jnp.max(own_l, axis=1, keepdims=True))
        cw[b] = c_exp.astype(BF16)
        qs[b] = jnp.broadcast_to(jnp.sum(c_exp, axis=1, keepdims=True), qs.shape[1:])

    own_pnt = pnt[pl.ds(pl.multiple_of(core * slots, slots), slots), :]
    near_tok = 4 * tok

    def slot_logits(b, half):
        rows = xn[b, 4 * half:4 * half + 4].reshape(near_tok, d_model)
        low, high = (lax.dot_general(own_pnt[:, d:d + half_d], rows[:, d:d + half_d], (((1,), (1,)), ((), ())),
                                     preferred_element_type=F32) for d in (0, half_d))
        lt = g * (low - high)
        lane = lax.broadcasted_iota(jnp.int32, lt.shape, 1)
        pos = lane
        for n, slot in enumerate(range(4 * half, 4 * half + 4)):
            owner = me if slot == 0 else owners[slot_of.index(slot)]
            pos = jnp.where(lane >= n * tok, lane + (owner - n) * tok, pos)
        return jnp.where(pos < len_ref[b], lt, NEG_FILL)

    def x_wait(rel, piece):
        x_send(0, piece, rel, part, 0).wait_recv()

    for piece in (0, 1):
        x_wait(1, piece)
        x_start(2, piece, 3, ynb, 3)
        if piece == 1:
            x_start(2, piece, 6, ysame, 6)
        x_start(2, piece, 4, part, 4)
        x_wait(2, piece + 2)
        x_start(3, piece + 2, 3, xnb, 3)
        if piece == 1:
            x_start(3, piece + 2, 6, xsame, 6)
        x_start(3, piece + 2, 5, part, 5)
    for piece in range(4):
        x_start(0, piece, 0, part, 0)
    for piece in range(4):
        x_wait(0, piece)
    normalise(1)
    for piece in (0, 1):
        x_wait(1, piece + 2)
        x_start(2, piece + 2, 4, part, 4)
        x_wait(2, piece)
        x_start(3, piece, 5, part, 5)
    normalise(2)
    normalise(3)
    for b in range(batch):
        la[b] = slot_logits(b, 0)
    for piece in (0, 2, 1, 3):
        x_wait(3, piece)
        if piece % 2 == 0:
            x_start(6, piece, 6, part, 6)
    for rel in (4, 5):
        for piece in range(4):
            x_wait(rel, piece)
    for slot in (4, 5, 6):
        normalise(slot)
    for piece in range(4):
        x_wait(6, piece)
    for b in range(batch):
        xn[b, 7] = row_normed(xg[b, 7])
        near, far = la[b], slot_logits(b, 1)
        top = jnp.maximum(jnp.max(near, axis=1, keepdims=True), jnp.max(far, axis=1, keepdims=True))
        d_exp = jnp.concatenate([jnp.exp(near - top), jnp.exp(far - top)], axis=1)
        z = jnp.sum(d_exp, axis=1, keepdims=True)
        tokens = xg[b].reshape(2 * near_tok, d_model)
        slot_sum = jnp.dot(d_exp.astype(BF16), tokens, preferred_element_type=F32)
        xs[b] = (slot_sum / z).astype(BF16).astype(F32)

    def y_rows(dev, e):
        return pl.ds(pl.multiple_of(dev * slots + e * per, per), per)

    def y_send(owner, e, rel, to, recv, cols=slice(None)):
        block = yg.at[:, y_rows(owner, e), cols]
        return pltpu.make_async_remote_copy(src_ref=block, dst_ref=block, send_sem=sy_sem.at[rel], recv_sem=recv,
                                            device_id={"seq": to}, device_id_type=MESH)

    def y_chunk(owner, e, c, rel, to, recv):
        return y_send(owner, e, rel, to, recv, pl.ds(c * width, width))

    def send_own(e, cols, recvs):
        for rel, to in ((3, dia), (1, xnb), (2, ynb), (0, part)):
            y_send(me, e, rel, to, recvs.at[rel], cols).start()

    def y_wait(e, rel):
        y_send(last_owners[rel], e, rel, part, ry_sem.at[e, rel]).wait_recv()

    def forward(e):
        for rel in (1, 2, 3):
            y_wait(e, rel)
            y_send(last_owners[rel], e, rel + 3, part, ry_sem.at[e, rel + 3]).start()

    fblk = 1024

    def hidden(e, slot, split=False):
        rows = xs[:, pl.ds(pl.multiple_of(e * per, per), per), :].reshape(batch * per, d_model)
        for f in range(ff // fblk):
            if split and f * fblk % (ff // 2) == 0:
                w1_last(2 * f * fblk // ff).wait()
            cols = pl.ds(f * fblk, fblk)
            up = jnp.dot(rows, w1b[slot, :, cols], preferred_element_type=F32)
            act = jax.nn.gelu(up).astype(BF16).astype(F32)
            h_v[:, cols] = -act if split and f * fblk >= ff // 2 else act

    def outputs(e, slot, cols):
        if cols.size > width:
            out = jnp.dot(h_v[...], w2b[slot, :, cols], preferred_element_type=F32)
        else:
            low, high = pl.ds(0, ff // 2), pl.ds(ff // 2, ff // 2)
            out = (jnp.dot(h_v[:, low], w2b[slot, low, cols], preferred_element_type=F32)
                   - jnp.dot(h_v[:, high], w2b[slot, high, cols], preferred_element_type=F32))
        out = out.astype(BF16)
        yg[:, y_rows(me, e), cols] = out.reshape(batch, per, cols.size)

    w1_copy(0).wait()
    hidden(0, 0)
    for half in (0, 1):
        w1_last(half).start(priority=1)
    w2_copy(0).wait()
    outputs(0, 0, pl.ds(0, d_model))
    send_own(0, pl.ds(0, d_model), ry_sem.at[0])
    for c in range(chunks):
        w2_last(c).start(priority=1)

    @pl.loop(1, last)
    def _(e):
        w1_copy(e).wait()
        hidden(e, e)
        w2_copy(e).wait()
        for c in range(2):
            outputs(e, e, pl.ds(c * 2 * width, 2 * width))
            send_own(e, pl.ds(c * 2 * width, 2 * width), ry_sem.at[e])

    forward(0)
    hidden(last, last % ring, True)
    for c in range(chunks):
        w2_last(c).wait()
        outputs(last, last % ring, pl.ds(c * width, width))
        send_own(last, pl.ds(c * width, width), rl_sem.at[c])
        if c == 1:
            for e in range(1, last - 1):
                forward(e)
    forward(last - 1)
    for c in range(chunks):
        for rel in (1, 2, 3):
            y_chunk(last_owners[rel], last, c, rel, part, rl_sem.at[c, rel]).wait_recv()
            y_chunk(last_owners[rel], last, c, rel + 3, part, rl_sem.at[c, rel + 3]).start()
    for e in range(last):
        for rel in (0, 4, 5, 6):
            y_wait(e, rel)
    def y_sent(rel):
        sent = yg.at[:, pl.ds(0, slots), :]
        pltpu.make_async_remote_copy(src_ref=sent, dst_ref=sent, send_sem=sy_sem.at[rel], recv_sem=ry_sem.at[0, rel],
                                     device_id={"seq": part}, device_id_type=MESH).wait_send()

    for copy in x_sends:
        copy.wait_send()
    for rel in range(4):
        y_sent(rel)
    first = me * tok
    for c in range(chunks):
        for rel in (0, 4, 5, 6):
            y_chunk(last_owners[rel], last, c, rel, part, rl_sem.at[c, rel]).wait_recv()
        cols = pl.ds(c * width, width)
        for b in range(batch):
            mixed = jnp.dot(cw[b], yg[b, :, cols], preferred_element_type=F32) / qs[b][:, :1]
            pos = first + lax.broadcasted_iota(jnp.int32, mixed.shape, 0)
            y_ref[b, :, cols] = jnp.where(pos < len_ref[b], mixed, 0.0).astype(BF16)

    for rel in (4, 5, 6):
        y_sent(rel)


def solution(mesh):
    seq_size = mesh.shape["seq"]

    def local_layer(tok_blk, len_blk, slot_param, logit_scale, w_in, w_out):
        batch, tok, d_model = tok_blk.shape
        n_slots = slot_param.shape[1]
        n_exp, _, ff = w_in.shape
        slots = n_slots // seq_size
        ring = n_exp - 1
        chunks = 4
        dma = pltpu.SemaphoreType.DMA
        sems = (dma, dma, dma((4,)), dma, dma((ring,)), dma((2,)), dma((ring,)), dma((chunks,)),
                dma((7, 4)), dma((7, 4)), dma((7,)), dma((n_exp, 7)), dma((chunks, 7)))
        return pl.pallas_call(
            functools.partial(layer_kernel, sems),
            out_shape=pltpu.VMEM((batch, tok, d_model), BF16),
            in_specs=[pl.BlockSpec(memory_space=pltpu.HBM)] * 6,
            out_specs=pl.BlockSpec(memory_space=pltpu.VMEM),
            scratch_shapes=[
                pltpu.VMEM((batch, seq_size, tok, d_model), BF16),
                pltpu.VMEM((batch, seq_size, tok, d_model), BF16),
                pltpu.VMEM((batch, slots, tok * seq_size // 2), F32),
                pltpu.VMEM((d_model, n_slots), BF16),
                pltpu.VMEM((d_model, n_slots), BF16),
                pltpu.VMEM((2 * slots, d_model), BF16),
                pltpu.VMEM((batch, slots, d_model), F32),
                pltpu.VMEM((batch * slots // n_exp, ff), F32),
                pltpu.VMEM((batch, n_slots, d_model), BF16),
                pltpu.VMEM((batch, tok, n_slots), BF16),
                pltpu.VMEM((batch, tok, 128), F32),
                pltpu.VMEM((ring, d_model, ff), BF16),
                pltpu.VMEM((ring, ff, d_model), BF16),
                pltpu.SMEM((batch,), jnp.int32),
                pltpu.SMEM((1,), F32),
            ],
            compiler_params=pltpu.CompilerParams(collective_id=0, has_side_effects=True, vmem_limit_bytes=60 * 1024 * 1024),
        )(len_blk, logit_scale.reshape(1), tok_blk, slot_param, w_in, w_out)

    return jax.shard_map(local_layer, mesh=mesh, in_specs=(P("data", "seq", None), P("data"), P(None, None), P(), P("seq", None, None), P("seq", None, None)), out_specs=P("data", "seq", None), check_vma=False)
```
